32 devices in a mesh: seq: 8 (over z, y), grp: 4 (over x, core).
Axes of the slice: x: 2, y: 2, z: 4, core: 2. Of those that a mesh axis runs over, the one named last changes fastest.
Arguments:
- queries: bfloat16 [8192, 1024], P(('seq', 'grp')), may hold values from -5 to 5
- key_rows: bfloat16 [8192, 128], P(('seq', 'grp')), may hold values from -5 to 5
- value_rows: bfloat16 [8192, 128], P(('seq', 'grp')), may hold values from -6 to 6
- out_grad: bfloat16 [8192, 1024], P(('seq', 'grp')), may hold values from -6 to 6
- segment: int32 [8192], P(('seq', 'grp')), may hold values from 0 to 9, never falling along the last dimension, each value on 1 to 1536 neighbouring positions
Outputs:
- attended: bfloat16 [8192, 1024], P(('seq', 'grp'))
- query_grad: bfloat16 [8192, 1024], P(('seq', 'grp'))
- key_grad: float32 [8192, 128], P(('seq', 'grp'))
- value_grad: float32 [8192, 128], P(('seq', 'grp'))
The draws below stay inside these ranges and needn't reach their ends.
Inputs may be any that keep to these rules, and one draw needn't show every extreme that they name: `segment`: segment numbers start at 0 and never fall along the sequence; every document holds 1 to 1536 tokens, and one holds exactly 1536.
All inputs are finite; a program needn't handle non-finite values.
Results may differ from the reference program's by a relative error of at most 0.019.
Values may be sent and summed in bfloat16 or wider, within the bound.
A program may use at most 64 MiB of HBM per device.

```python
import math
import jax
import jax.numpy as jnp
import numpy as np
from jax import lax

HEADS = 8
HD = 128
TOK_DEV = 256
MAXDOC = 1536
TOKENS = 8192
SEGMENTS = 10


def pair_draw(key):
    base = jax.random.fold_in(key, 7)
    streams = jax.random.split(base, 2)
    query_draw = jnp.clip(jax.random.normal(streams[0], (TOKENS, HEADS * HD), jnp.float32), -5.0, 5.0)
    key_draw = jnp.clip(jax.random.normal(streams[1], (TOKENS, HD), jnp.float32), -5.0, 5.0)
    return (query_draw, key_draw)


def draw_queries(key, part):
    return pair_draw(key)[0].astype(jnp.bfloat16)


def draw_key_rows(key, part):
    return pair_draw(key)[1].astype(jnp.bfloat16)


def steps_of(own_key, shape, pieces, smallest, high):
    factor_of = 1.0
    for axis_at, parts in pieces:
        draws = jax.random.uniform(jax.random.fold_in(jax.random.fold_in(own_key, 6), axis_at), (parts,), jnp.float32, smallest / len(pieces), high / len(pieces))
        factor_of = factor_of * jnp.repeat(jnp.exp(draws), shape[axis_at] // parts).reshape((-1,) + (1,) * (len(shape) - 1 - axis_at))
    return factor_of


def length_profile(count, total, bound, slope):
    loads = [(1 << 20) // math.isqrt(standing ** slope) + 1 for standing in range(2, count + 1)]
    rest, counts = total - bound - (count - 1), [1] * (count - 1)
    while rest > 0:
        free = [i for i in range(count - 1) if counts[i] < bound]
        whole, budget = sum([loads[i] for i in free]), rest
        for i in free:
            addition = min(bound - counts[i], max(1, budget * loads[i] // whole), rest)
            counts[i] = counts[i] + addition
            rest = rest - addition
    return np.array([bound] + counts)


def ragged(own_key, count, total, limit, slope):
    if count == 2:
        one = jax.random.randint(own_key, (), max(1, total - limit), min(limit, total - 1) + 1)
        return jnp.stack([one, total - one])
    tallies = jnp.asarray(length_profile(count, total, limit, slope), jnp.int32)
    couples = (count - 1) // 2
    donor, sink = tallies[1:1 + 2 * couples:2], tallies[2:2 + 2 * couples:2]
    room = jnp.minimum(donor - 1, limit - sink)
    shifted = jax.random.randint(jax.random.fold_in(own_key, 1), (couples,), 0, 1 << 20) % (room + 1)
    tallies = tallies.at[1:1 + 2 * couples:2].set(donor - shifted).at[2:2 + 2 * couples:2].set(sink + shifted)
    return tallies[jax.random.permutation(jax.random.fold_in(own_key, 2), count)]


def normal_values(key, extent, scale, most, cuts=(), kind=jnp.bfloat16):
    result = scale * jax.random.normal(key, extent, jnp.float32)
    if cuts:
        result = result * steps_of(key, extent, cuts, -0.22, 0.18)
    return jnp.clip(result, -most, most).astype(kind)


def setup_inputs(seed: int = 0) -> dict:
    seeds = jax.random.split(jax.random.key(seed), 6)
    queries = draw_queries(jax.random.fold_in(seeds[5], 71), 0)
    key_rows = draw_key_rows(jax.random.fold_in(seeds[5], 71), 0)
    value_rows = normal_values(seeds[2], (TOKENS, HD), 1.0, 6.0, ((0, 32),))
    out_grad = normal_values(seeds[3], (TOKENS, HEADS * HD), 1.0, 6.0, ((0, 32),))
    segment = jnp.searchsorted(jnp.cumsum(ragged(seeds[4], SEGMENTS, TOKENS, MAXDOC, 1)), jnp.arange(TOKENS), side="right").astype(jnp.int32)
    return dict(queries=queries, key_rows=key_rows, value_rows=value_rows, out_grad=out_grad, segment=segment)


def reference(queries, key_rows, value_rows, out_grad, segment):
    score_scale = HD ** -0.5
    block_rows = 512 if TOKENS % 512 == 0 else TOK_DEV
    block_count = TOKENS // block_rows
    window = MAXDOC + block_rows
    keys_padded = jnp.concatenate([jnp.zeros((MAXDOC, HD), key_rows.dtype), key_rows], axis=0)
    values_padded = jnp.concatenate([jnp.zeros((MAXDOC, HD), value_rows.dtype), value_rows], axis=0)
    segment_padded = jnp.concatenate([jnp.full((MAXDOC,), -1, jnp.int32), segment.astype(jnp.int32)], axis=0)

    def one_block(running, index):
        key_total, value_total = running
        start = (index * block_rows).astype(jnp.int32)
        query_block = lax.dynamic_slice_in_dim(queries, start, block_rows, 0).astype(jnp.float32).reshape(block_rows, HEADS, HD)
        grad_block = lax.dynamic_slice_in_dim(out_grad, start, block_rows, 0).astype(jnp.float32).reshape(block_rows, HEADS, HD)
        query_seg = lax.dynamic_slice_in_dim(segment.astype(jnp.int32), start, block_rows, 0)
        key_window = lax.dynamic_slice_in_dim(keys_padded, start, window, 0).astype(jnp.float32)
        value_window = lax.dynamic_slice_in_dim(values_padded, start, window, 0).astype(jnp.float32)
        key_seg = lax.dynamic_slice_in_dim(segment_padded, start, window, 0)
        query_pos = start + jnp.arange(block_rows, dtype=jnp.int32)
        key_pos = start - MAXDOC + jnp.arange(window, dtype=jnp.int32)
        visible = (key_seg[None, :] == query_seg[:, None]) & (key_pos[None, :] <= query_pos[:, None])
        visible = visible[:, None, :]
        scores = jnp.einsum("thd,kd->thk", query_block, key_window) * score_scale
        row_max = jnp.max(jnp.where(visible, scores, -1e30), axis=-1)
        row_sum = jnp.sum(jnp.where(visible, jnp.exp(scores - row_max[..., None]), 0.0), axis=-1)
        log_total = row_max + jnp.log(row_sum)
        prob = jnp.where(visible, jnp.exp(scores - log_total[..., None]), 0.0)
        weight = prob.astype(jnp.bfloat16)
        attended = jnp.einsum("thk,kd->thd", weight.astype(jnp.float32), value_window).astype(jnp.bfloat16)
        row_dot = jnp.sum(grad_block * attended.astype(jnp.float32), axis=-1)
        dprob = jnp.einsum("thd,kd->thk", grad_block, value_window)
        dscore = (score_scale * prob * (dprob - row_dot[..., None])).astype(jnp.bfloat16)
        query_grad = jnp.einsum("thk,kd->thd", dscore.astype(jnp.float32), key_window).astype(jnp.bfloat16)
        key_part = jnp.einsum("thk,thd->kd", dscore.astype(jnp.float32), query_block)
        value_part = jnp.einsum("thk,thd->kd", weight.astype(jnp.float32), grad_block)
        key_total = lax.dynamic_update_slice_in_dim(key_total, lax.dynamic_slice_in_dim(key_total, start, window, 0) + key_part, start, 0)
        value_total = lax.dynamic_update_slice_in_dim(value_total, lax.dynamic_slice_in_dim(value_total, start, window, 0) + value_part, start, 0)
        return (key_total, value_total), (attended.reshape(block_rows, HEADS * HD), query_grad.reshape(block_rows, HEADS * HD))

    start_totals = (jnp.zeros((MAXDOC + TOKENS, HD), jnp.float32), jnp.zeros((MAXDOC + TOKENS, HD), jnp.float32))
    totals, outputs = lax.scan(one_block, start_totals, jnp.arange(block_count, dtype=jnp.int32))
    attended = outputs[0].reshape(TOKENS, HEADS * HD)
    query_grad = outputs[1].reshape(TOKENS, HEADS * HD)
    return attended, query_grad, totals[0][MAXDOC:], totals[1][MAXDOC:]
```

```python
import functools
import math

import jax
import jax.numpy as jnp
from jax import lax
from jax.experimental import pallas as pl
from jax.experimental.pallas import tpu as pltpu
from jax.sharding import PartitionSpec as P

MAXDOC = 1536
AXES = ("seq", "grp")
MESH = pl.DeviceIdType.MESH
F32 = jnp.float32
BF16 = jnp.bfloat16
HIDDEN = -1e30


def dot_nt(a, b):
    return lax.dot_general(a, b, (((1,), (1,)), ((), ())), preferred_element_type=F32)


def dot_nn(a, b):
    return lax.dot_general(a, b, (((1,), (0,)), ((), ())), preferred_element_type=F32)


def kernel(
    groups, total, span,
    q_hbm, k_hbm, v_hbm, g_hbm, seg_hbm,
    o_hbm, dq_hbm, dk_hbm, dv_hbm,
    keys, values, segs, qs, gs, gt, bias, probs, o_buf, dq_buf, dk_buf, dv_buf,
    row_max, tops, sums, row_dot,
    gk_odd, gv_odd, gk_pair, gv_pair, gk_out, gv_out, gk_in, gv_in,
    local, o_sem, dq_sem, d_sem,
    k_send, k_recv, s_send, s_recv, v_send, v_recv, kf_send, vf_send,
    gkp_send, gkp_recv, gvp_send, gvp_recv, gk_send, gk_recv, gv_send, gv_recv,
):
    tokens, width = k_hbm.shape
    heads = q_hbm.shape[1] // width
    half = span // 2
    scale = width ** -0.5
    exponent = scale * math.log2(math.e)
    me = lax.axis_index("seq") * groups + lax.axis_index("grp")
    parity = lax.rem(me, 2)
    partner = me + 1 - 2 * parity

    def at(where):
        return (lax.div(where, groups), lax.rem(where, groups))

    def rows(d):
        return pl.ds(pl.multiple_of(d * tokens, tokens), tokens)

    def remote(src, dst, send, recv, where):
        return pltpu.make_async_remote_copy(
            src_ref=src, dst_ref=dst, send_sem=send, recv_sem=recv,
            device_id=at(where), device_id_type=MESH)

    def key_copy(d):
        return remote(keys.at[rows(0)], keys.at[rows(d)], k_send.at[d], k_recv.at[d], me + d)

    def value_copy(d):
        return remote(values.at[rows(0)], values.at[rows(d)], v_send.at[d], v_recv.at[d], me + d)

    def seg_copy(d):
        return remote(segs.at[0], segs.at[d], s_send.at[d], s_recv.at[d], me + d)

    def key_pass_on(j):
        return remote(keys.at[rows(2 * j + 2 * parity)], keys.at[rows(2 * j + 1)],
                      kf_send.at[j], k_recv.at[2 * j + 1], partner)

    def value_pass_on(j):
        return remote(values.at[rows(2 * j + 2 * parity)], values.at[rows(2 * j + 1)],
                      vf_send.at[j], v_recv.at[2 * j + 1], partner)

    def pair_copy(odd, pair, send, recv, j):
        return remote(odd.at[j], pair.at[j], send.at[j], recv.at[j], partner)

    def total_copy(out, into, send, recv, j):
        return remote(out.at[j], into.at[j], send.at[j], recv.at[j], me - 2 * (j + 1))

    barrier = pltpu.get_barrier_semaphore()
    expected = 0
    for d in range(1, span + 1):
        for way in (d, -d):
            inside = (me + way >= 0) & (me + way < total)
            expected = expected + inside.astype(jnp.int32)

            @pl.when(inside)
            def _():
                pl.semaphore_signal(barrier, inc=1, device_id=at(me + way), device_id_type=MESH)

    key_load = pltpu.make_async_copy(k_hbm, keys.at[pl.ds(0, tokens)], local.at[0])
    seg_load = pltpu.make_async_copy(seg_hbm, segs.at[0], local.at[1])
    value_load = pltpu.make_async_copy(v_hbm, values.at[pl.ds(0, tokens)], local.at[2])
    key_load.start()
    seg_load.start()
    value_load.start()
    loads_q = []
    loads_g = []
    for h in range(heads):
        stacked = pl.ds(h * tokens, tokens)
        head = pl.ds(h * width, width)
        loads_q.append(pltpu.make_async_copy(q_hbm.at[:, head], qs.at[stacked], local.at[3 + h]))
        loads_g.append(pltpu.make_async_copy(g_hbm.at[:, head], gs.at[stacked], local.at[3 + heads + h]))
    for load in loads_q + loads_g:
        load.start()

    for d in range(1, span + 1):
        @pl.when(me < d)
        def _():
            keys[pl.ds(d * tokens, tokens), :] = jnp.zeros((tokens, width), BF16)
            values[pl.ds(d * tokens, tokens), :] = jnp.zeros((tokens, width), BF16)
            segs[d] = jnp.zeros((1, tokens), jnp.int32)

    key_load.wait()
    seg_load.wait()
    value_load.wait()
    pl.semaphore_wait(barrier, expected)

    @pl.when(parity == 0)
    def _():
        key_pass_on(0).start()

    for d in range(2, span + 1, 2):
        @pl.when(me + d < total)
        def _():
            key_copy(d).start()

    for d in range(1, span + 1):
        @pl.when(me + d < total)
        def _():
            seg_copy(d).start()

    @pl.when(parity == 0)
    def _():
        value_pass_on(0).start()

    for d in range(2, span + 1, 2):
        @pl.when(me + d < total)
        def _():
            value_copy(d).start()

    row_max[...] = jnp.full(row_max.shape, HIDDEN, F32)
    for load in loads_q + loads_g:
        load.wait()
    for h in range(heads):
        stacked = pl.ds(h * tokens, tokens)
        gt[:, stacked] = gs[stacked, :].T

    def score_pass(s, carry):
        odd = lax.rem(s, 2)
        d = jnp.where(s == 0, 0, s + 2 * odd - 1)
        j = lax.div(d, 2) - parity

        @pl.when((d > 0) & (me >= d))
        def _():
            key_copy(d).wait_recv()
            seg_copy(d).wait_recv()

        @pl.when((odd == 1) & (me >= d) & (j < half))
        def _():
            key_pass_on(j).start()

        key_block = keys[rows(d), :]
        seg_column = jnp.broadcast_to(segs[d].astype(F32), (128, tokens)).T
        seg_key = jnp.concatenate([seg_column] * (tokens // 128), axis=1)
        key_at = lax.broadcasted_iota(jnp.int32, (tokens, tokens), 0) - d * tokens
        query_at = lax.broadcasted_iota(jnp.int32, (tokens, tokens), 1)
        first = jnp.where(me >= d, -d * tokens, tokens)
        visible = (seg_key == segs[0].astype(F32)) & (key_at <= query_at) & (key_at >= first)
        bias[...] = jnp.where(visible, 0.0, HIDDEN)
        for h in range(heads):
            cols = pl.ds(h * tokens, tokens)
            score = dot_nt(key_block, qs[cols, :]) + bias[...]
            top = jnp.max(score, axis=0, keepdims=True)
            top = jnp.maximum(row_max[0:1, cols], top)
            part = jnp.exp2((score - top) * exponent)
            row_max[:, cols] = jnp.broadcast_to(top, (8, tokens))
            tops[d, :, cols] = jnp.broadcast_to(top, (8, tokens))
            sums[d, :, cols] = jnp.sum(part.reshape(tokens // 8, 8, tokens), axis=0)
            probs[rows(d), cols] = part.astype(BF16)
        return carry

    lax.fori_loop(0, span + 1, score_pass, 0)
    for h in range(heads):
        cols = pl.ds(h * tokens, tokens)
        whole = jnp.zeros((8, tokens), F32)
        for d in range(span + 1):
            part = jnp.exp2((tops[d, :, cols] - row_max[:, cols]) * exponent)
            tops[d, :, cols] = part
            whole += part * sums[d, :, cols]
        inverse = jnp.broadcast_to(1.0 / jnp.sum(whole, axis=0, keepdims=True), (8, tokens))
        for d in range(span + 1):
            tops[d, :, cols] *= inverse

    order = [d for m in range(half, 0, -1) for d in (2 * m - 1, 2 * m)]
    order = [5, 3, 6, 1, 4, 2, 0] if span == 6 else order + [0]

    def block_at(s):
        d = order[-1]
        for i in range(len(order) - 1):
            d = jnp.where(s == i, order[i], d)
        return d

    def hand_out(d, part, odd_ref, pair_ref, out_ref, sum_ref, p_send, p_recv, t_send, into, t_recv):
        sum_ref[...] = part
        j = lax.div(d, 2)
        is_odd = lax.rem(d, 2) == 1

        @pl.when(is_odd & (me >= d))
        def _():
            odd_ref[j] = sum_ref[...].astype(BF16)
            pair_copy(odd_ref, pair_ref, p_send, p_recv, j).start()

        i = j - parity

        @pl.when(jnp.logical_not(is_odd) & (me >= d) & (i >= 0) & (i < half))
        def _():
            pair_copy(odd_ref, pair_ref, p_send, p_recv, i).wait_recv()
            sum_ref[...] += pair_ref[i].astype(F32)

        @pl.when(jnp.logical_not(is_odd) & (d > 0) & (me >= d))
        def _():
            out_ref[j - 1] = sum_ref[...].astype(BF16)
            total_copy(out_ref, into, t_send, t_recv, j - 1).start()

    def value_grad_pass(s, carry):
        d = block_at(s)
        e = 2 * s + 2

        @pl.when((s < half) & (me >= e))
        def _():
            value_copy(e).wait_recv()

        @pl.when((s < half) & (me >= e) & (s + 1 - parity < half))
        def _():
            value_pass_on(s + 1 - parity).start()

        for h in range(heads):
            cols = pl.ds(h * tokens, tokens)
            prob = probs[rows(d), cols].astype(F32) * tops[d, 0:1, cols]
            probs[rows(d), cols] = prob.astype(BF16)
        part = dot_nn(probs[rows(d), :], gs[...])
        hand_out(d, part, gv_odd, gv_pair, gv_out, dv_buf, gvp_send, gvp_recv, gv_send, gv_in, gv_recv)
        return carry

    lax.fori_loop(0, span + 1, value_grad_pass, 0)
    for d in range(1, span + 1, 2):
        @pl.when(me >= d)
        def _():
            value_copy(d).wait_recv()

    values_t = values[...].T
    o_copies = []
    for h in range(heads):
        cols = pl.ds(h * tokens, tokens)
        head = pl.ds(h * width, width)
        attended = dot_nn(values_t, probs[:, cols]).astype(BF16)
        dot = jnp.sum(attended.astype(F32) * gt[:, cols].astype(F32), axis=0, keepdims=True)
        row_dot[:, cols] = jnp.broadcast_to(dot, (8, tokens))
        o_buf[:, head] = attended.T
    o_copy = pltpu.make_async_copy(o_buf, o_hbm, o_sem)
    o_copy.start()

    def key_grad_pass(s, carry):
        d = block_at(s)
        value_block = values[rows(d), :]
        for h in range(heads):
            cols = pl.ds(h * tokens, tokens)
            dprob = dot_nt(value_block, gs[cols, :])
            prob = probs[rows(d), cols].astype(F32)
            probs[rows(d), cols] = (prob * (dprob - row_dot[0:1, cols])).astype(BF16)
        part = dot_nn(probs[rows(d), :], qs[...]) * scale
        hand_out(d, part, gk_odd, gk_pair, gk_out, dk_buf, gkp_send, gkp_recv, gk_send, gk_in, gk_recv)
        return carry

    lax.fori_loop(0, span + 1, key_grad_pass, 0)
    keys_t = keys[...].T
    for h in range(heads):
        cols = pl.ds(h * tokens, tokens)
        grad = (dot_nn(keys_t, probs[:, cols]) * scale).astype(BF16)
        dq_buf[:, pl.ds(h * width, width)] = grad.T
    dq_copy = pltpu.make_async_copy(dq_buf, dq_hbm, dq_sem)
    dq_copy.start()

    for j in range(half - 1, -1, -1):
        @pl.when(me + 2 * (j + 1) < total)
        def _():
            total_copy(gv_out, gv_in, gv_send, gv_recv, j).wait_recv()
            dv_buf[...] += gv_in[j].astype(F32)

    dv_copy = pltpu.make_async_copy(dv_buf, dv_hbm, d_sem.at[0])
    dv_copy.start()
    for j in range(half - 1, -1, -1):
        @pl.when(me + 2 * (j + 1) < total)
        def _():
            total_copy(gk_out, gk_in, gk_send, gk_recv, j).wait_recv()
            dk_buf[...] += gk_in[j].astype(F32)

    dk_copy = pltpu.make_async_copy(dk_buf, dk_hbm, d_sem.at[1])
    dk_copy.start()

    for d in range(1, span + 1):
        @pl.when(me + d < total)
        def _():
            seg_copy(d).wait_send()
            if d % 2 == 0:
                key_copy(d).wait_send()
                value_copy(d).wait_send()
    for j in range(half):
        @pl.when(me >= 2 * j + 2 * parity)
        def _():
            key_pass_on(j).wait_send()
            value_pass_on(j).wait_send()

        @pl.when(me >= 2 * j + 1)
        def _():
            pair_copy(gv_odd, gv_pair, gvp_send, gvp_recv, j).wait_send()
            pair_copy(gk_odd, gk_pair, gkp_send, gkp_recv, j).wait_send()

        @pl.when(me >= 2 * j + 2)
        def _():
            total_copy(gv_out, gv_in, gv_send, gv_recv, j).wait_send()
            total_copy(gk_out, gk_in, gk_send, gk_recv, j).wait_send()
    o_copy.wait()
    dq_copy.wait()
    dv_copy.wait()
    dk_copy.wait()


def on_device(queries, key_rows, value_rows, out_grad, segment):
    tokens, width = key_rows.shape
    heads = queries.shape[1] // width
    groups = lax.axis_size("grp")
    total = groups * lax.axis_size("seq")
    span = -(-MAXDOC // tokens)
    span += span % 2
    blocks = span + 1
    half = span // 2
    stacked = heads * tokens
    seg_rows = segment.reshape(1, tokens)
    anywhere = pl.BlockSpec(memory_space=pl.ANY)
    sem = pltpu.SemaphoreType.DMA
    block = pltpu.VMEM((half, tokens, width), BF16)
    return pl.pallas_call(
        functools.partial(kernel, groups, total, span),
        out_shape=(
            jax.ShapeDtypeStruct(queries.shape, BF16),
            jax.ShapeDtypeStruct(queries.shape, BF16),
            jax.ShapeDtypeStruct(key_rows.shape, F32),
            jax.ShapeDtypeStruct(key_rows.shape, F32),
        ),
        in_specs=[anywhere] * 5,
        out_specs=(anywhere,) * 4,
        scratch_shapes=[
            pltpu.VMEM((blocks * tokens, width), BF16),
            pltpu.VMEM((blocks * tokens, width), BF16),
            pltpu.VMEM((blocks, 1, tokens), jnp.int32),
            pltpu.VMEM((stacked, width), BF16),
            pltpu.VMEM((stacked, width), BF16),
            pltpu.VMEM((width, stacked), BF16),
            pltpu.VMEM((tokens, tokens), F32),
            pltpu.VMEM((blocks * tokens, stacked), BF16),
            pltpu.VMEM(queries.shape, BF16),
            pltpu.VMEM(queries.shape, BF16),
            pltpu.VMEM(key_rows.shape, F32),
            pltpu.VMEM(key_rows.shape, F32),
            pltpu.VMEM((8, stacked), F32),
            pltpu.VMEM((blocks, 8, stacked), F32),
            pltpu.VMEM((blocks, 8, stacked), F32),
            pltpu.VMEM((8, stacked), F32),
        ]
        + [block] * 8
        + [sem((3 + 2 * heads,)), sem, sem, sem((2,))]
        + [sem((blocks,))] * 6
        + [sem((half,))] * 10,
        compiler_params=pltpu.CompilerParams(
            collective_id=0, has_side_effects=True, vmem_limit_bytes=60 * 1024 * 1024
        ),
    )(queries, key_rows, value_rows, out_grad, seg_rows)


def solution(mesh):
    in_specs = (P(AXES, None), P(AXES, None), P(AXES, None), P(AXES, None), P(AXES))
    out_specs = (P(AXES, None),) * 4
    return jax.shard_map(
        on_device, mesh=mesh, in_specs=in_specs, out_specs=out_specs, check_vma=False
    )
```

```python
import functools
import math

import jax
import jax.numpy as jnp
from jax import lax
from jax.experimental import pallas as pl
from jax.experimental.pallas import tpu as pltpu
from jax.sharding import PartitionSpec as P

MAXDOC = 1536
AXES = ("seq", "grp")
MESH = pl.DeviceIdType.MESH
F32 = jnp.float32
BF16 = jnp.bfloat16
HIDDEN = -1e30


def dot_nt(a, b):
    return lax.dot_general(a, b, (((1,), (1,)), ((), ())), preferred_element_type=F32)


def dot_nn(a, b):
    return lax.dot_general(a, b, (((1,), (0,)), ((), ())), preferred_element_type=F32)


def kernel(
    groups, total, span,
    q_hbm, k_hbm, v_hbm, g_hbm, seg_hbm,
    o_buf, dq_buf, dk_buf, dv_buf,
    keys, values, segs, qs, gs, gt, bias, probs,
    row_max, tops, sums, row_dot,
    gk_odd, gv_odd, gk_pair, gv_pair, gk_out, gv_out, gk_in, gv_in,
    local,
    k_send, k_recv, s_send, s_recv, v_send, v_recv, kf_send, vf_send,
    gkp_send, gkp_recv, gvp_send, gvp_recv, gk_send, gk_recv, gv_send, gv_recv,
):
    tokens, width = k_hbm.shape
    heads = q_hbm.shape[1] // width
    half = span // 2
    scale = width ** -0.5
    exponent = scale * math.log2(math.e)
    me = lax.axis_index("seq") * groups + lax.axis_index("grp")
    parity = lax.rem(me, 2)
    partner = me + 1 - 2 * parity

    def at(where):
        return (lax.div(where, groups), lax.rem(where, groups))

    def rows(d):
        return pl.ds(pl.multiple_of(d * tokens, tokens), tokens)

    def remote(src, dst, send, recv, where):
        return pltpu.make_async_remote_copy(
            src_ref=src, dst_ref=dst, send_sem=send, recv_sem=recv,
            device_id=at(where), device_id_type=MESH)

    def key_copy(d):
        return remote(keys.at[rows(0)], keys.at[rows(d)], k_send.at[d], k_recv.at[d], me + d)

    def value_copy(d):
        return remote(values.at[rows(0)], values.at[rows(d)], v_send.at[d], v_recv.at[d], me + d)

    def seg_copy(d):
        return remote(segs.at[0], segs.at[d], s_send.at[d], s_recv.at[d], me + d)

    def key_pass_on(j):
        return remote(keys.at[rows(2 * j + 2 * parity)], keys.at[rows(2 * j + 1)],
                      kf_send.at[j], k_recv.at[2 * j + 1], partner)

    def value_pass_on(j):
        return remote(values.at[rows(2 * j + 2 * parity)], values.at[rows(2 * j + 1)],
                      vf_send.at[j], v_recv.at[2 * j + 1], partner)

    def pair_copy(odd, pair, send, recv, j):
        return remote(odd.at[j], pair.at[j], send.at[j], recv.at[j], partner)

    def total_copy(out, into, send, recv, j):
        return remote(out.at[j], into.at[j], send.at[j], recv.at[j], me - 2 * (j + 1))

    barrier = pltpu.get_barrier_semaphore()
    expected = 0
    for d in range(1, span + 1):
        for way in (d, -d):
            inside = (me + way >= 0) & (me + way < total)
            expected = expected + inside.astype(jnp.int32)

            @pl.when(inside)
            def _():
                pl.semaphore_signal(barrier, inc=1, device_id=at(me + way), device_id_type=MESH)

    key_load = pltpu.make_async_copy(k_hbm, keys.at[pl.ds(0, tokens)], local.at[0])
    seg_load = pltpu.make_async_copy(seg_hbm, segs.at[0], local.at[1])
    value_load = pltpu.make_async_copy(v_hbm, values.at[pl.ds(0, tokens)], local.at[2])
    key_load.start()
    seg_load.start()
    value_load.start()
    loads_q = []
    loads_g = []
    for h in range(heads):
        stacked = pl.ds(h * tokens, tokens)
        head = pl.ds(h * width, width)
        loads_q.append(pltpu.make_async_copy(q_hbm.at[:, head], qs.at[stacked], local.at[3 + h]))
        loads_g.append(pltpu.make_async_copy(g_hbm.at[:, head], gs.at[stacked], local.at[3 + heads + h]))
    for load in loads_q + loads_g:
        load.start()

    for d in range(1, span + 1):
        @pl.when(me < d)
        def _():
            keys[pl.ds(d * tokens, tokens), :] = jnp.zeros((tokens, width), BF16)
            values[pl.ds(d * tokens, tokens), :] = jnp.zeros((tokens, width), BF16)
            segs[d] = jnp.zeros((1, tokens), jnp.int32)

    key_load.wait()
    seg_load.wait()
    value_load.wait()
    pl.semaphore_wait(barrier, expected)

    @pl.when(parity == 0)
    def _():
        key_pass_on(0).start()

    for d in range(2, span + 1, 2):
        @pl.when(me + d < total)
        def _():
            key_copy(d).start()

    for d in range(1, span + 1):
        @pl.when(me + d < total)
        def _():
            seg_copy(d).start()

    @pl.when(parity == 0)
    def _():
        value_pass_on(0).start()

    for d in range(2, span + 1, 2):
        @pl.when(me + d < total)
        def _():
            value_copy(d).start()

    row_max[...] = jnp.full(row_max.shape, HIDDEN, F32)
    for load in loads_q + loads_g:
        load.wait()
    for h in range(heads):
        stacked = pl.ds(h * tokens, tokens)
        gt[:, stacked] = gs[stacked, :].T

    def score_pass(s, carry):
        odd = lax.rem(s, 2)
        d = jnp.where(s == 0, 0, s + 2 * odd - 1)
        j = lax.div(d, 2) - parity

        @pl.when((d > 0) & (me >= d))
        def _():
            key_copy(d).wait_recv()
            seg_copy(d).wait_recv()

        @pl.when((odd == 1) & (me >= d) & (j < half))
        def _():
            key_pass_on(j).start()

        key_block = keys[rows(d), :]
        seg_column = jnp.broadcast_to(segs[d].astype(F32), (128, tokens)).T
        seg_key = jnp.concatenate([seg_column] * (tokens // 128), axis=1)
        key_at = lax.broadcasted_iota(jnp.int32, (tokens, tokens), 0) - d * tokens
        query_at = lax.broadcasted_iota(jnp.int32, (tokens, tokens), 1)
        first = jnp.where(me >= d, -d * tokens, tokens)
        visible = (seg_key == segs[0].astype(F32)) & (key_at <= query_at) & (key_at >= first)
        bias[...] = jnp.where(visible, 0.0, HIDDEN)
        for h in range(heads):
            cols = pl.ds(h * tokens, tokens)
            score = dot_nt(key_block, qs[cols, :]) + bias[...]
            top = jnp.max(score, axis=0, keepdims=True)
            top = jnp.maximum(row_max[0:1, cols], top)
            part = jnp.exp2((score - top) * exponent)
            row_max[:, cols] = jnp.broadcast_to(top, (8, tokens))
            tops[d, :, cols] = jnp.broadcast_to(top, (8, tokens))
            sums[d, :, cols] = jnp.sum(part.reshape(tokens // 8, 8, tokens), axis=0)
            probs[rows(d), cols] = part.astype(BF16)
        return carry

    lax.fori_loop(0, span + 1, score_pass, 0)
    for h in range(heads):
        cols = pl.ds(h * tokens, tokens)
        whole = jnp.zeros((8, tokens), F32)
        for d in range(span + 1):
            part = jnp.exp2((tops[d, :, cols] - row_max[:, cols]) * exponent)
            tops[d, :, cols] = part
            whole += part * sums[d, :, cols]
        inverse = jnp.broadcast_to(1.0 / jnp.sum(whole, axis=0, keepdims=True), (8, tokens))
        for d in range(span + 1):
            tops[d, :, cols] *= inverse

    order = [d for m in range(half, 0, -1) for d in (2 * m - 1, 2 * m)]
    order = [5, 3, 6, 1, 4, 2, 0] if span == 6 else order + [0]

    def block_at(s):
        d = order[-1]
        for i in range(len(order) - 1):
            d = jnp.where(s == i, order[i], d)
        return d

    def hand_out(d, part, odd_ref, pair_ref, out_ref, sum_ref, p_send, p_recv, t_send, into, t_recv):
        sum_ref[...] = part
        j = lax.div(d, 2)
        is_odd = lax.rem(d, 2) == 1

        @pl.when(is_odd & (me >= d))
        def _():
            odd_ref[j] = sum_ref[...].astype(BF16)
            pair_copy(odd_ref, pair_ref, p_send, p_recv, j).start()

        i = j - parity

        @pl.when(jnp.logical_not(is_odd) & (me >= d) & (i >= 0) & (i < half))
        def _():
            pair_copy(odd_ref, pair_ref, p_send, p_recv, i).wait_recv()
            sum_ref[...] += pair_ref[i].astype(F32)

        @pl.when(jnp.logical_not(is_odd) & (d > 0) & (me >= d))
        def _():
            out_ref[j - 1] = sum_ref[...].astype(BF16)
            total_copy(out_ref, into, t_send, t_recv, j - 1).start()

    def value_grad_pass(s, carry):
        d = block_at(s)
        e = 2 * s + 2

        @pl.when((s < half) & (me >= e))
        def _():
            value_copy(e).wait_recv()

        @pl.when((s < half) & (me >= e) & (s + 1 - parity < half))
        def _():
            value_pass_on(s + 1 - parity).start()

        for h in range(heads):
            cols = pl.ds(h * tokens, tokens)
            prob = probs[rows(d), cols].astype(F32) * tops[d, 0:1, cols]
            probs[rows(d), cols] = prob.astype(BF16)
        part = dot_nn(probs[rows(d), :], gs[...])
        hand_out(d, part, gv_odd, gv_pair, gv_out, dv_buf, gvp_send, gvp_recv, gv_send, gv_in, gv_recv)
        return carry

    lax.fori_loop(0, span + 1, value_grad_pass, 0)
    for d in range(1, span + 1, 2):
        @pl.when(me >= d)
        def _():
            value_copy(d).wait_recv()

    values_t = values[...].T
    for h in range(heads):
        cols = pl.ds(h * tokens, tokens)
        head = pl.ds(h * width, width)
        attended = dot_nn(values_t, probs[:, cols]).astype(BF16)
        dot = jnp.sum(attended.astype(F32) * gt[:, cols].astype(F32), axis=0, keepdims=True)
        row_dot[:, cols] = jnp.broadcast_to(dot, (8, tokens))
        o_buf[:, head] = attended.T

    def key_grad_pass(s, carry):
        d = block_at(s)
        value_block = values[rows(d), :]
        for h in range(heads):
            cols = pl.ds(h * tokens, tokens)
            dprob = dot_nt(value_block, gs[cols, :])
            prob = probs[rows(d), cols].astype(F32)
            probs[rows(d), cols] = (prob * (dprob - row_dot[0:1, cols])).astype(BF16)
        part = dot_nn(probs[rows(d), :], qs[...]) * scale
        hand_out(d, part, gk_odd, gk_pair, gk_out, dk_buf, gkp_send, gkp_recv, gk_send, gk_in, gk_recv)
        return carry

    lax.fori_loop(0, span + 1, key_grad_pass, 0)
    keys_t = keys[...].T
    for h in range(heads):
        cols = pl.ds(h * tokens, tokens)
        grad = (dot_nn(keys_t, probs[:, cols]) * scale).astype(BF16)
        dq_buf[:, pl.ds(h * width, width)] = grad.T

    for j in range(half - 1, -1, -1):
        @pl.when(me + 2 * (j + 1) < total)
        def _():
            total_copy(gv_out, gv_in, gv_send, gv_recv, j).wait_recv()
            dv_buf[...] += gv_in[j].astype(F32)

    for j in range(half - 1, -1, -1):
        @pl.when(me + 2 * (j + 1) < total)
        def _():
            total_copy(gk_out, gk_in, gk_send, gk_recv, j).wait_recv()
            dk_buf[...] += gk_in[j].astype(F32)


    for d in range(1, span + 1):
        @pl.when(me + d < total)
        def _():
            seg_copy(d).wait_send()
            if d % 2 == 0:
                key_copy(d).wait_send()
                value_copy(d).wait_send()
    for j in range(half):
        @pl.when(me >= 2 * j + 2 * parity)
        def _():
            key_pass_on(j).wait_send()
            value_pass_on(j).wait_send()

        @pl.when(me >= 2 * j + 1)
        def _():
            pair_copy(gv_odd, gv_pair, gvp_send, gvp_recv, j).wait_send()
            pair_copy(gk_odd, gk_pair, gkp_send, gkp_recv, j).wait_send()

        @pl.when(me >= 2 * j + 2)
        def _():
            total_copy(gv_out, gv_in, gv_send, gv_recv, j).wait_send()
            total_copy(gk_out, gk_in, gk_send, gk_recv, j).wait_send()


def on_device(queries, key_rows, value_rows, out_grad, segment):
    tokens, width = key_rows.shape
    heads = queries.shape[1] // width
    groups = lax.axis_size("grp")
    total = groups * lax.axis_size("seq")
    span = -(-MAXDOC // tokens)
    span += span % 2
    blocks = span + 1
    half = span // 2
    stacked = heads * tokens
    seg_rows = segment.reshape(1, tokens)
    anywhere = pl.BlockSpec(memory_space=pl.ANY)
    sem = pltpu.SemaphoreType.DMA
    block = pltpu.VMEM((half, tokens, width), BF16)
    results = pl.pallas_call(
        functools.partial(kernel, groups, total, span),
        out_shape=(
            pltpu.VMEM(queries.shape, BF16),
            pltpu.VMEM(queries.shape, BF16),
            pltpu.VMEM(key_rows.shape, F32),
            pltpu.VMEM(key_rows.shape, F32),
        ),
        in_specs=[anywhere] * 5,
        out_specs=(pl.BlockSpec(memory_space=pltpu.VMEM),) * 4,
        scratch_shapes=[
            pltpu.VMEM((blocks * tokens, width), BF16),
            pltpu.VMEM((blocks * tokens, width), BF16),
            pltpu.VMEM((blocks, 1, tokens), jnp.int32),
            pltpu.VMEM((stacked, width), BF16),
            pltpu.VMEM((stacked, width), BF16),
            pltpu.VMEM((width, stacked), BF16),
            pltpu.VMEM((tokens, tokens), F32),
            pltpu.VMEM((blocks * tokens, stacked), BF16),
            pltpu.VMEM((8, stacked), F32),
            pltpu.VMEM((blocks, 8, stacked), F32),
            pltpu.VMEM((blocks, 8, stacked), F32),
            pltpu.VMEM((8, stacked), F32),
        ]
        + [block] * 8
        + [sem((3 + 2 * heads,))]
        + [sem((blocks,))] * 6
        + [sem((half,))] * 10,
        compiler_params=pltpu.CompilerParams(
            collective_id=0, has_side_effects=True, vmem_limit_bytes=40 * 1024 * 1024
        ),
    )(*[
        pltpu.with_memory_space_constraint(a, pltpu.HBM)
        for a in (queries, key_rows, value_rows, out_grad, seg_rows)
    ])
    return write_back(results)


def store(*refs):
    count = (len(refs) - 1) // 2
    copies = [pltpu.make_async_copy(refs[i], refs[count + i], refs[-1].at[i]) for i in range(count)]
    for copy in copies:
        copy.start()
    for copy in copies:
        copy.wait()


def write_back(results):
    anywhere = pl.BlockSpec(memory_space=pl.ANY)
    held = [pltpu.with_memory_space_constraint(r, pltpu.VMEM) for r in results]
    return pl.pallas_call(
        store,
        out_shape=tuple(jax.ShapeDtypeStruct(r.shape, r.dtype) for r in results),
        in_specs=[pl.BlockSpec(memory_space=pltpu.VMEM)] * len(results),
        out_specs=(anywhere,) * len(results),
        scratch_shapes=[pltpu.SemaphoreType.DMA((len(results),))],
        compiler_params=pltpu.CompilerParams(vmem_limit_bytes=4 * 1024 * 1024),
    )(*held)


def solution(mesh):
    in_specs = (P(AXES, None), P(AXES, None), P(AXES, None), P(AXES, None), P(AXES))
    out_specs = (P(AXES, None),) * 4
    return jax.shard_map(
        on_device, mesh=mesh, in_specs=in_specs, out_specs=out_specs, check_vma=False
    )
```

```python
import functools
import math

import jax
import jax.numpy as jnp
from jax import lax
from jax.experimental import pallas as pl
from jax.experimental.pallas import tpu as pltpu
from jax.sharding import PartitionSpec as P

MAXDOC = 1536
AXES = ("seq", "grp")
MESH = pl.DeviceIdType.MESH
F32 = jnp.float32
BF16 = jnp.bfloat16
HIDDEN = -1e30
SAME = 8192.0


def dot_nt(a, b):
    return lax.dot_general(a, b, (((1,), (1,)), ((), ())), preferred_element_type=F32)


def dot_nn(a, b):
    return lax.dot_general(a, b, (((1,), (0,)), ((), ())), preferred_element_type=F32)


def kernel(
    groups, total, span,
    q_hbm, k_hbm, v_hbm, g_hbm, seg_hbm,
    o_buf, dq_buf, dk_buf, dv_buf,
    keys, values, segs, qs, gs, qt, gt, hots, marks_t, scores, probs, dscores, value_parts,
    row_max, row_inv, row_dot,
    gk_odd, gv_odd, gk_pair, gv_pair, gk_out, gv_out, gk_in, gv_in,
    local,
    k_send, k_recv, s_send, s_recv, v_send, v_recv, kf_send, vf_send,
    gkp_send, gkp_recv, gvp_send, gvp_recv, gk_send, gk_recv, gv_send, gv_recv,
):
    tokens, width = k_hbm.shape
    heads = q_hbm.shape[1] // width
    half = span // 2
    scale = width ** -0.5
    exponent = scale * math.log2(math.e)
    me = lax.axis_index("seq") * groups + lax.axis_index("grp")
    parity = lax.rem(me, 2)
    partner = me + 1 - 2 * parity

    def at(where):
        return (lax.div(where, groups), lax.rem(where, groups))

    def rows(d):
        return pl.ds(pl.multiple_of(d * tokens, tokens), tokens)

    def remote(src, dst, send, recv, where):
        return pltpu.make_async_remote_copy(
            src_ref=src, dst_ref=dst, send_sem=send, recv_sem=recv,
            device_id=at(where), device_id_type=MESH)

    def key_copy(d):
        return remote(keys.at[rows(0)], keys.at[rows(d)], k_send.at[d], k_recv.at[d], me + d)

    def value_copy(d):
        return remote(values.at[rows(0)], values.at[rows(d)], v_send.at[d], v_recv.at[d], me + d)

    def seg_copy(d):
        return remote(segs.at[0], segs.at[d], s_send.at[d], s_recv.at[d], me + d)

    def key_pass_on(j):
        return remote(keys.at[rows(2 * j + 2 * parity)], keys.at[rows(2 * j + 1)],
                      kf_send.at[j], k_recv.at[2 * j + 1], partner)

    def value_pass_on(j):
        return remote(values.at[rows(2 * j + 2 * parity)], values.at[rows(2 * j + 1)],
                      vf_send.at[j], v_recv.at[2 * j + 1], partner)

    def pair_copy(odd, pair, send, recv, j):
        return remote(odd.at[j], pair.at[j], send.at[j], recv.at[j], partner)

    def total_copy(out, into, send, recv, j):
        return remote(out.at[j], into.at[j], send.at[j], recv.at[j], me - 2 * (j + 1))

    barrier = pltpu.get_barrier_semaphore()
    expected = 0
    for d in range(1, span + 1):
        for way in (d, -d):
            inside = (me + way >= 0) & (me + way < total)
            expected = expected + inside.astype(jnp.int32)

            @pl.when(inside)
            def _():
                pl.semaphore_signal(barrier, inc=1, device_id=at(me + way), device_id_type=MESH)

    key_load = pltpu.make_async_copy(k_hbm, keys.at[pl.ds(0, tokens)], local.at[0])
    seg_load = pltpu.make_async_copy(seg_hbm, segs.at[0], local.at[1])
    value_load = pltpu.make_async_copy(v_hbm, values.at[pl.ds(0, tokens)], local.at[2])
    key_load.start()
    seg_load.start()
    value_load.start()
    loads_q = []
    loads_g = []
    for h in range(heads):
        stacked = pl.ds(h * tokens, tokens)
        head = pl.ds(h * width, width)
        loads_q.append(pltpu.make_async_copy(q_hbm.at[:, head], qs.at[stacked], local.at[3 + h]))
        loads_g.append(pltpu.make_async_copy(g_hbm.at[:, head], gs.at[stacked], local.at[3 + heads + h]))
    for load in loads_q + loads_g:
        load.start()

    for d in range(1, span + 1):
        @pl.when(me < d)
        def _():
            keys[pl.ds(d * tokens, tokens), :] = jnp.zeros((tokens, width), BF16)
            values[pl.ds(d * tokens, tokens), :] = jnp.zeros((tokens, width), BF16)
            hots[pl.ds(d * tokens, tokens), :] = jnp.zeros((tokens, width), BF16)

    key_load.wait()
    seg_load.wait()
    value_load.wait()
    pl.semaphore_wait(barrier, expected)

    @pl.when(parity == 0)
    def _():
        key_pass_on(0).start()

    for d in range(2, span + 1, 2):
        @pl.when(me + d < total)
        def _():
            key_copy(d).start()

    for d in range(1, span + 1):
        @pl.when(me + d < total)
        def _():
            seg_copy(d).start()

    @pl.when(parity == 0)
    def _():
        value_pass_on(0).start()

    def one_hot(d):
        column = jnp.broadcast_to((segs[d] & (width - 1)).astype(F32), (width, tokens)).T
        lane = lax.broadcasted_iota(jnp.int32, (tokens, width), 1).astype(F32)
        return jnp.where(column == lane, 1.0, 0.0)

    for load in loads_q + loads_g:
        load.wait()
    for h in range(heads):
        stacked = pl.ds(h * tokens, tokens)
        qt[:, stacked] = qs[stacked, :].T
        gt[:, stacked] = gs[stacked, :].T

    own_hot = one_hot(0)
    hots[pl.ds(0, tokens), :] = own_hot.astype(BF16)
    marks_t[...] = (own_hot * SAME).astype(BF16).T
    row_max[...] = jnp.full(row_max.shape, HIDDEN, F32)

    def score_block(d, diagonal):
        key_block = jnp.concatenate([keys[rows(d), :], hots[rows(d), :]], axis=1)
        for h in range(heads):
            cols = pl.ds(h * tokens, tokens)
            query = jnp.concatenate([qt[:, cols], marks_t[...]], axis=0)
            score = dot_nn(key_block, query) * exponent
            if diagonal:
                key_at = lax.broadcasted_iota(jnp.int32, (tokens, tokens), 0)
                query_at = lax.broadcasted_iota(jnp.int32, (tokens, tokens), 1)
                score = jnp.where(key_at <= query_at, score, HIDDEN)
            scores[rows(d), cols] = score
            top = jnp.max(score.reshape(tokens // 8, 8, tokens), axis=0)
            row_max[:, cols] = jnp.maximum(row_max[:, cols], top)

    score_block(0, True)

    def score_pass(s, carry):
        odd = lax.rem(s, 2)
        d = s + 2 * odd - 1
        j = lax.div(d, 2) - parity

        @pl.when(me >= d)
        def _():
            key_copy(d).wait_recv()
            seg_copy(d).wait_recv()
            hots[rows(d), :] = one_hot(d).astype(BF16)

        @pl.when((odd == 1) & (me >= d) & (j < half))
        def _():
            key_pass_on(j).start()

        for e in range(2, span + 1, 2):
            @pl.when((s == 1) & (me + e < total))
            def _():
                value_copy(e).start()

        score_block(d, False)
        return carry

    lax.fori_loop(1, span + 1, score_pass, 0)
    ones = jnp.ones((16, (span + 1) * tokens), BF16)
    group = 2 * tokens

    def exp_block(h, d, top):
        block = pl.ds(d * tokens, tokens)
        cols = pl.ds(h * tokens, tokens)
        probs[block, cols] = jnp.exp2(scores[block, cols] - top).astype(BF16)

    def normalise(h):
        cols = pl.ds(h * tokens, tokens)
        inverse = 1.0 / dot_nn(ones, probs[:, cols])[0:1, :]
        row_inv[:, cols] = jnp.broadcast_to(inverse, (8, tokens))
        scaled = (gt[:, cols].astype(F32) * inverse).astype(BF16)
        gt[:, cols] = scaled
        gs[cols, :] = scaled.T

    def value_grad(i, d):
        block = pl.ds(d * tokens, tokens)
        cols = pl.ds(i * group, group)
        part = dot_nn(probs[block, cols], gs[cols, :])
        if i > 0:
            part += value_parts[block, :]
        value_parts[block, :] = part

    for i in range(heads // 2):
        e = 2 * i + 2
        if e <= span:
            @pl.when(me >= e)
            def _():
                value_copy(e).wait_recv()

            @pl.when((me >= e) & (e // 2 - parity < half))
            def _():
                value_pass_on(e // 2 - parity).start()

        pair = (2 * i, 2 * i + 1)
        peaks = [jnp.max(row_max[:, pl.ds(h * tokens, tokens)], axis=0, keepdims=True) for h in pair]
        for d in range(span + 1):
            if i > 0:
                value_grad(i - 1, d)
            for h, top in zip(pair, peaks):
                exp_block(h, d, top)
        for h in pair:
            normalise(h)
    for d in range(span + 1):
        value_grad(heads // 2 - 1, d)
    for e in range(heads + 2, span + 1, 2):
        @pl.when(me >= e)
        def _():
            value_copy(e).wait_recv()

        @pl.when((me >= e) & (e // 2 - parity < half))
        def _():
            value_pass_on(e // 2 - parity).start()

    order = [d for m in range(half, 0, -1) for d in (2 * m - 1, 2 * m)]
    order = [5, 3, 6, 1, 4, 2, 0] if span == 6 else order + [0]

    def block_at(s):
        d = order[-1]
        for i in range(len(order) - 1):
            d = jnp.where(s == i, order[i], d)
        return d

    def hand_out(d, part, odd_ref, pair_ref, out_ref, sum_ref, p_send, p_recv, t_send, into, t_recv):
        sum_ref[...] = part
        j = lax.div(jnp.int32(d), 2)
        is_odd = lax.rem(jnp.int32(d), 2) == 1

        @pl.when(is_odd & (me >= d))
        def _():
            odd_ref[j] = sum_ref[...].astype(BF16)
            pair_copy(odd_ref, pair_ref, p_send, p_recv, j).start()

        i = j - parity

        @pl.when(jnp.logical_not(is_odd) & (me >= d) & (i >= 0) & (i < half))
        def _():
            pair_copy(odd_ref, pair_ref, p_send, p_recv, i).wait_recv()
            sum_ref[...] += pair_ref[i].astype(F32)

        @pl.when(jnp.logical_not(is_odd) & (d > 0) & (me >= d))
        def _():
            out_ref[j - 1] = sum_ref[...].astype(BF16)
            total_copy(out_ref, into, t_send, t_recv, j - 1).start()

    def value_hand_out(d):
        hand_out(d, value_parts[rows(d), :], gv_odd, gv_pair, gv_out, dv_buf,
                 gvp_send, gvp_recv, gv_send, gv_in, gv_recv)

    for d in range(span - 1, 0, -2):
        value_hand_out(d)
    for d in range(1, span + 1, 2):
        @pl.when(me >= d)
        def _():
            value_copy(d).wait_recv()

    values_t = values[...].T
    for h in range(heads):
        cols = pl.ds(h * tokens, tokens)
        head = pl.ds(h * width, width)
        attended = (dot_nn(values_t, probs[:, cols]) * row_inv[0:1, cols]).astype(BF16)
        dot = jnp.sum(attended.astype(F32) * gt[:, cols].astype(F32), axis=0, keepdims=True)
        row_dot[:, cols] = jnp.broadcast_to(dot, (8, tokens))
        o_buf[:, head] = attended.T

    for d in range(span, -1, -2):
        value_hand_out(d)

    def key_grad_pass(s, carry):
        d = block_at(s)
        value_block = values[rows(d), :]
        for h in range(heads):
            cols = pl.ds(h * tokens, tokens)
            dprob = dot_nn(value_block, gt[:, cols])
            prob = probs[rows(d), cols].astype(F32)
            dscores[rows(d), cols] = (prob * (dprob - row_dot[0:1, cols])).astype(BF16)
        part = dot_nn(dscores[rows(d), :], qs[...]) * scale
        hand_out(d, part, gk_odd, gk_pair, gk_out, dk_buf, gkp_send, gkp_recv, gk_send, gk_in, gk_recv)
        return carry

    lax.fori_loop(0, span + 1, key_grad_pass, 0)
    keys_t = keys[...].T
    for h in range(heads):
        cols = pl.ds(h * tokens, tokens)
        grad = (dot_nn(keys_t, dscores[:, cols]) * scale).astype(BF16)
        dq_buf[:, pl.ds(h * width, width)] = grad.T

    for j in range(half - 1, -1, -1):
        @pl.when(me + 2 * (j + 1) < total)
        def _():
            total_copy(gv_out, gv_in, gv_send, gv_recv, j).wait_recv()
            dv_buf[...] += gv_in[j].astype(F32)

    for j in range(half - 1, -1, -1):
        @pl.when(me + 2 * (j + 1) < total)
        def _():
            total_copy(gk_out, gk_in, gk_send, gk_recv, j).wait_recv()
            dk_buf[...] += gk_in[j].astype(F32)


    for d in range(1, span + 1):
        @pl.when(me + d < total)
        def _():
            seg_copy(d).wait_send()
            if d % 2 == 0:
                key_copy(d).wait_send()
                value_copy(d).wait_send()
    for j in range(half):
        @pl.when(me >= 2 * j + 2 * parity)
        def _():
            key_pass_on(j).wait_send()
            value_pass_on(j).wait_send()

        @pl.when(me >= 2 * j + 1)
        def _():
            pair_copy(gv_odd, gv_pair, gvp_send, gvp_recv, j).wait_send()
            pair_copy(gk_odd, gk_pair, gkp_send, gkp_recv, j).wait_send()

        @pl.when(me >= 2 * j + 2)
        def _():
            total_copy(gv_out, gv_in, gv_send, gv_recv, j).wait_send()
            total_copy(gk_out, gk_in, gk_send, gk_recv, j).wait_send()


def on_device(queries, key_rows, value_rows, out_grad, segment):
    tokens, width = key_rows.shape
    heads = queries.shape[1] // width
    groups = lax.axis_size("grp")
    total = groups * lax.axis_size("seq")
    span = -(-MAXDOC // tokens)
    span += span % 2
    blocks = span + 1
    half = span // 2
    stacked = heads * tokens
    seg_rows = segment.reshape(1, tokens)
    anywhere = pl.BlockSpec(memory_space=pl.ANY)
    sem = pltpu.SemaphoreType.DMA
    block = pltpu.VMEM((half, tokens, width), BF16)
    results = pl.pallas_call(
        functools.partial(kernel, groups, total, span),
        out_shape=(
            pltpu.VMEM(queries.shape, BF16),
            pltpu.VMEM(queries.shape, BF16),
            pltpu.VMEM(key_rows.shape, F32),
            pltpu.VMEM(key_rows.shape, F32),
        ),
        in_specs=[anywhere] * 5,
        out_specs=(pl.BlockSpec(memory_space=pltpu.VMEM),) * 4,
        scratch_shapes=[
            pltpu.VMEM((blocks * tokens, width), BF16),
            pltpu.VMEM((blocks * tokens, width), BF16),
            pltpu.VMEM((blocks, 1, tokens), jnp.int32),
            pltpu.VMEM((stacked, width), BF16),
            pltpu.VMEM((stacked, width), BF16),
            pltpu.VMEM((width, stacked), BF16),
            pltpu.VMEM((width, stacked), BF16),
            pltpu.VMEM((blocks * tokens, width), BF16),
            pltpu.VMEM((width, tokens), BF16),
            pltpu.VMEM((blocks * tokens, stacked), F32),
            pltpu.VMEM((blocks * tokens, stacked), BF16),
            pltpu.VMEM((blocks * tokens, stacked), BF16),
            pltpu.VMEM((blocks * tokens, width), F32),
            pltpu.VMEM((8, stacked), F32),
            pltpu.VMEM((8, stacked), F32),
            pltpu.VMEM((8, stacked), F32),
        ]
        + [block] * 8
        + [sem((3 + 2 * heads,))]
        + [sem((blocks,))] * 6
        + [sem((half,))] * 10,
        compiler_params=pltpu.CompilerParams(
            collective_id=0, has_side_effects=True, vmem_limit_bytes=48 * 1024 * 1024
        ),
    )(*[
        pltpu.with_memory_space_constraint(a, pltpu.HBM)
        for a in (queries, key_rows, value_rows, out_grad, seg_rows)
    ])
    return write_back(results)


def store(*refs):
    count = (len(refs) - 1) // 2
    copies = [pltpu.make_async_copy(refs[i], refs[count + i], refs[-1].at[i]) for i in range(count)]
    for copy in copies:
        copy.start()
    for copy in copies:
        copy.wait()


def write_back(results):
    anywhere = pl.BlockSpec(memory_space=pl.ANY)
    held = [pltpu.with_memory_space_constraint(r, pltpu.VMEM) for r in results]
    return pl.pallas_call(
        store,
        out_shape=tuple(jax.ShapeDtypeStruct(r.shape, r.dtype) for r in results),
        in_specs=[pl.BlockSpec(memory_space=pltpu.VMEM)] * len(results),
        out_specs=(anywhere,) * len(results),
        scratch_shapes=[pltpu.SemaphoreType.DMA((len(results),))],
        compiler_params=pltpu.CompilerParams(vmem_limit_bytes=4 * 1024 * 1024),
    )(*held)


def solution(mesh):
    in_specs = (P(AXES, None), P(AXES, None), P(AXES, None), P(AXES, None), P(AXES))
    out_specs = (P(AXES, None),) * 4
    return jax.shard_map(
        on_device, mesh=mesh, in_specs=in_specs, out_specs=out_specs, check_vma=False
    )
```

```python
import functools
import math

import jax
import jax.numpy as jnp
from jax import lax
from jax.experimental import pallas as pl
from jax.experimental.pallas import tpu as pltpu
from jax.sharding import PartitionSpec as P

MAXDOC = 1536
AXES = ("seq", "grp")
MESH = pl.DeviceIdType.MESH
F32 = jnp.float32
BF16 = jnp.bfloat16
HIDDEN = -1e30
SAME = 8192.0


def dot_nt(a, b):
    return lax.dot_general(a, b, (((1,), (1,)), ((), ())), preferred_element_type=F32)


def dot_nn(a, b):
    return lax.dot_general(a, b, (((1,), (0,)), ((), ())), preferred_element_type=F32)


def kernel(
    groups, total, span,
    q_hbm, k_hbm, v_hbm, g_hbm, seg_hbm,
    o_buf, dq_buf, dk_buf, dv_buf,
    keys, values, segs, qs, gs, qt, gt, hots, marks_t, scores, probs, dscores, value_parts,
    row_max, row_inv, row_dot,
    gk_odd, gv_odd, gk_pair, gv_pair, gk_out, gv_out, gk_in, gv_in,
    local,
    k_send, k_recv, s_send, s_recv, v_send, v_recv, kf_send, vf_send,
    gkp_send, gkp_recv, gvp_send, gvp_recv, gk_send, gk_recv, gv_send, gv_recv,
):
    tokens, width = k_hbm.shape
    heads = q_hbm.shape[1] // width
    half = span // 2
    scale = width ** -0.5
    exponent = scale * math.log2(math.e)
    me = lax.axis_index("seq") * groups + lax.axis_index("grp")
    parity = lax.rem(me, 2)
    partner = me + 1 - 2 * parity

    def at(where):
        return (lax.div(where, groups), lax.rem(where, groups))

    def rows(d):
        return pl.ds(pl.multiple_of(d * tokens, tokens), tokens)

    def remote(src, dst, send, recv, where):
        return pltpu.make_async_remote_copy(
            src_ref=src, dst_ref=dst, send_sem=send, recv_sem=recv,
            device_id=at(where), device_id_type=MESH)

    def key_copy(d):
        return remote(keys.at[rows(0)], keys.at[rows(d)], k_send.at[d], k_recv.at[d], me + d)

    def value_copy(d):
        return remote(values.at[rows(0)], values.at[rows(d)], v_send.at[d], v_recv.at[d], me + d)

    def seg_copy(d):
        return remote(segs.at[0], segs.at[d], s_send.at[d], s_recv.at[d], me + d)

    def key_pass_on(j):
        return remote(keys.at[rows(2 * j + 2 * parity)], keys.at[rows(2 * j + 1)],
                      kf_send.at[j], k_recv.at[2 * j + 1], partner)

    def value_pass_on(j):
        return remote(values.at[rows(2 * j + 2 * parity)], values.at[rows(2 * j + 1)],
                      vf_send.at[j], v_recv.at[2 * j + 1], partner)

    def pair_copy(odd, pair, send, recv, j):
        return remote(odd.at[j], pair.at[j], send.at[j], recv.at[j], partner)

    def total_copy(out, into, send, recv, j):
        return remote(out.at[j], into.at[j], send.at[j], recv.at[j], me - 2 * (j + 1))

    barrier = pltpu.get_barrier_semaphore()
    expected = 0
    for d in range(1, span + 1):
        for way in (d, -d):
            inside = (me + way >= 0) & (me + way < total)
            expected = expected + inside.astype(jnp.int32)

            @pl.when(inside)
            def _():
                pl.semaphore_signal(barrier, inc=1, device_id=at(me + way), device_id_type=MESH)

    key_load = pltpu.make_async_copy(k_hbm, keys.at[pl.ds(0, tokens)], local.at[0])
    seg_load = pltpu.make_async_copy(seg_hbm, segs.at[0], local.at[1])
    value_load = pltpu.make_async_copy(v_hbm, values.at[pl.ds(0, tokens)], local.at[2])
    key_load.start()
    seg_load.start()
    value_load.start()
    loads_q = []
    loads_g = []
    for h in range(heads):
        stacked = pl.ds(h * tokens, tokens)
        head = pl.ds(h * width, width)
        loads_q.append(pltpu.make_async_copy(q_hbm.at[:, head], qs.at[stacked], local.at[3 + h]))
        loads_g.append(pltpu.make_async_copy(g_hbm.at[:, head], gs.at[stacked], local.at[3 + heads + h]))
    for load in loads_q + loads_g:
        load.start()

    for d in range(1, span + 1):
        @pl.when(me < d)
        def _():
            keys[pl.ds(d * tokens, tokens), :] = jnp.zeros((tokens, width), BF16)
            values[pl.ds(d * tokens, tokens), :] = jnp.zeros((tokens, width), BF16)
            hots[pl.ds(d * tokens, tokens), :] = jnp.zeros((tokens, width), BF16)

    key_load.wait()
    seg_load.wait()
    value_load.wait()
    pl.semaphore_wait(barrier, expected)

    for d in range(1, span + 1):
        @pl.when(me + d < total)
        def _():
            seg_copy(d).start()

    @pl.when(parity == 0)
    def _():
        key_pass_on(0).start()

    for d in range(2, span + 1, 2):
        @pl.when(me + d < total)
        def _():
            key_copy(d).start()

    @pl.when(parity == 0)
    def _():
        value_pass_on(0).start()

    def one_hot(d):
        column = jnp.broadcast_to((segs[d] & (width - 1)).astype(F32), (width, tokens)).T
        lane = lax.broadcasted_iota(jnp.int32, (tokens, width), 1).astype(F32)
        return jnp.where(column == lane, 1.0, 0.0)

    for e in range(2, span + 1, 2):
        @pl.when(me + e < total)
        def _():
            value_copy(e).start()

    for load in loads_q + loads_g:
        load.wait()
    for h in range(heads):
        stacked = pl.ds(h * tokens, tokens)
        qt[:, stacked] = qs[stacked, :].T
        gt[:, stacked] = gs[stacked, :].T

    own_hot = one_hot(0)
    hots[pl.ds(0, tokens), :] = own_hot.astype(BF16)
    marks_t[...] = (own_hot * SAME).astype(BF16).T
    row_max[...] = jnp.full(row_max.shape, HIDDEN, F32)

    def score_block(d, diagonal):
        key_block = jnp.concatenate([keys[rows(d), :], hots[rows(d), :]], axis=1)
        for h in range(heads):
            cols = pl.ds(h * tokens, tokens)
            query = jnp.concatenate([qt[:, cols], marks_t[...]], axis=0)
            score = dot_nn(key_block, query) * exponent
            if diagonal:
                key_at = lax.broadcasted_iota(jnp.int32, (tokens, tokens), 0)
                query_at = lax.broadcasted_iota(jnp.int32, (tokens, tokens), 1)
                score = jnp.where(key_at <= query_at, score, HIDDEN)
            scores[rows(d), cols] = score
            top = jnp.max(score.reshape(tokens // 8, 8, tokens), axis=0)
            row_max[:, cols] = jnp.maximum(row_max[:, cols], top)

    score_block(0, True)

    def score_pass(s, carry):
        direct = s <= half
        d = jnp.where(direct, 2 * s, 2 * (s - half) - 1)
        j = s - parity

        @pl.when(me >= d)
        def _():
            key_copy(d).wait_recv()
            seg_copy(d).wait_recv()
            hots[rows(d), :] = one_hot(d).astype(BF16)

        @pl.when(direct & (me >= d) & (j < half))
        def _():
            key_pass_on(j).start()

        score_block(d, False)
        return carry

    lax.fori_loop(1, span + 1, score_pass, 0)
    ones = jnp.ones((16, (span + 1) * tokens), BF16)
    group = 2 * tokens

    def exp_block(h, d, top):
        block = pl.ds(d * tokens, tokens)
        cols = pl.ds(h * tokens, tokens)
        probs[block, cols] = jnp.exp2(scores[block, cols] - top).astype(BF16)

    def normalise(h):
        cols = pl.ds(h * tokens, tokens)
        inverse = 1.0 / dot_nn(ones, probs[:, cols])[0:1, :]
        row_inv[:, cols] = jnp.broadcast_to(inverse, (8, tokens))
        scaled = (gt[:, cols].astype(F32) * inverse).astype(BF16)
        gt[:, cols] = scaled
        gs[cols, :] = scaled.T

    def value_grad(i, d):
        block = pl.ds(d * tokens, tokens)
        cols = pl.ds(i * group, group)
        part = dot_nn(probs[block, cols], gs[cols, :])
        if i > 0:
            part += value_parts[block, :]
        value_parts[block, :] = part

    for i in range(heads // 2):
        e = 2 * i + 2
        if e <= span:
            @pl.when(me >= e)
            def _():
                value_copy(e).wait_recv()

            @pl.when((me >= e) & (e // 2 - parity < half))
            def _():
                value_pass_on(e // 2 - parity).start()

        pair = (2 * i, 2 * i + 1)
        peaks = [jnp.max(row_max[:, pl.ds(h * tokens, tokens)], axis=0, keepdims=True) for h in pair]
        for d in range(span + 1):
            if i > 0:
                value_grad(i - 1, d)
            for h, top in zip(pair, peaks):
                exp_block(h, d, top)
        for h in pair:
            normalise(h)
    for d in range(span + 1):
        value_grad(heads // 2 - 1, d)
    for e in range(heads + 2, span + 1, 2):
        @pl.when(me >= e)
        def _():
            value_copy(e).wait_recv()

        @pl.when((me >= e) & (e // 2 - parity < half))
        def _():
            value_pass_on(e // 2 - parity).start()

    order = [d for m in range(half, 0, -1) for d in (2 * m - 1, 2 * m)]
    order = [5, 3, 6, 1, 4, 2, 0] if span == 6 else order + [0]

    def block_at(s):
        d = order[-1]
        for i in range(len(order) - 1):
            d = jnp.where(s == i, order[i], d)
        return d

    def hand_out(d, part, odd_ref, pair_ref, out_ref, sum_ref, p_send, p_recv, t_send, into, t_recv):
        sum_ref[...] = part
        j = lax.div(jnp.int32(d), 2)
        is_odd = lax.rem(jnp.int32(d), 2) == 1

        @pl.when(is_odd & (me >= d))
        def _():
            odd_ref[j] = sum_ref[...].astype(BF16)
            pair_copy(odd_ref, pair_ref, p_send, p_recv, j).start()

        i = j - parity

        @pl.when(jnp.logical_not(is_odd) & (me >= d) & (i >= 0) & (i < half))
        def _():
            pair_copy(odd_ref, pair_ref, p_send, p_recv, i).wait_recv()
            sum_ref[...] += pair_ref[i].astype(F32)

        @pl.when(jnp.logical_not(is_odd) & (d > 0) & (me >= d))
        def _():
            out_ref[j - 1] = sum_ref[...].astype(BF16)
            total_copy(out_ref, into, t_send, t_recv, j - 1).start()

    def value_hand_out(d):
        hand_out(d, value_parts[rows(d), :], gv_odd, gv_pair, gv_out, dv_buf,
                 gvp_send, gvp_recv, gv_send, gv_in, gv_recv)

    for d in range(span - 1, 0, -2):
        value_hand_out(d)
    for d in range(1, span + 1, 2):
        @pl.when(me >= d)
        def _():
            value_copy(d).wait_recv()

    values_t = values[...].T
    for h in range(heads):
        cols = pl.ds(h * tokens, tokens)
        head = pl.ds(h * width, width)
        attended = (dot_nn(values_t, probs[:, cols]) * row_inv[0:1, cols]).astype(BF16)
        dot = jnp.sum(attended.astype(F32) * gt[:, cols].astype(F32), axis=0, keepdims=True)
        row_dot[:, cols] = jnp.broadcast_to(dot, (8, tokens))
        o_buf[:, head] = attended.T
        if h == heads // 2 - 1:
            for d in range(span, -1, -2):
                value_hand_out(d)

    def key_grad_pass(s, carry):
        d = block_at(s)
        value_block = values[rows(d), :]
        for h in range(heads):
            cols = pl.ds(h * tokens, tokens)
            dprob = dot_nn(value_block, gt[:, cols])
            prob = probs[rows(d), cols].astype(F32)
            dscores[rows(d), cols] = (prob * (dprob - row_dot[0:1, cols])).astype(BF16)
        part = dot_nn(dscores[rows(d), :], qs[...]) * scale
        hand_out(d, part, gk_odd, gk_pair, gk_out, dk_buf, gkp_send, gkp_recv, gk_send, gk_in, gk_recv)
        return carry

    lax.fori_loop(0, span + 1, key_grad_pass, 0)
    keys_t = keys[...].T
    for h in range(heads):
        cols = pl.ds(h * tokens, tokens)
        grad = (dot_nn(keys_t, dscores[:, cols]) * scale).astype(BF16)
        dq_buf[:, pl.ds(h * width, width)] = grad.T

    for j in range(half - 1, -1, -1):
        @pl.when(me + 2 * (j + 1) < total)
        def _():
            total_copy(gv_out, gv_in, gv_send, gv_recv, j).wait_recv()
            dv_buf[...] += gv_in[j].astype(F32)

    for j in range(half - 1, -1, -1):
        @pl.when(me + 2 * (j + 1) < total)
        def _():
            total_copy(gk_out, gk_in, gk_send, gk_recv, j).wait_recv()
            dk_buf[...] += gk_in[j].astype(F32)


    for d in range(1, span + 1):
        @pl.when(me + d < total)
        def _():
            seg_copy(d).wait_send()
            if d % 2 == 0:
                key_copy(d).wait_send()
                value_copy(d).wait_send()
    for j in range(half):
        @pl.when(me >= 2 * j + 2 * parity)
        def _():
            key_pass_on(j).wait_send()
            value_pass_on(j).wait_send()

        @pl.when(me >= 2 * j + 1)
        def _():
            pair_copy(gv_odd, gv_pair, gvp_send, gvp_recv, j).wait_send()
            pair_copy(gk_odd, gk_pair, gkp_send, gkp_recv, j).wait_send()

        @pl.when(me >= 2 * j + 2)
        def _():
            total_copy(gv_out, gv_in, gv_send, gv_recv, j).wait_send()
            total_copy(gk_out, gk_in, gk_send, gk_recv, j).wait_send()


def on_device(queries, key_rows, value_rows, out_grad, segment):
    tokens, width = key_rows.shape
    heads = queries.shape[1] // width
    groups = lax.axis_size("grp")
    total = groups * lax.axis_size("seq")
    span = -(-MAXDOC // tokens)
    span += span % 2
    blocks = span + 1
    half = span // 2
    stacked = heads * tokens
    seg_rows = segment.reshape(1, tokens)
    anywhere = pl.BlockSpec(memory_space=pl.ANY)
    sem = pltpu.SemaphoreType.DMA
    block = pltpu.VMEM((half, tokens, width), BF16)
    results = pl.pallas_call(
        functools.partial(kernel, groups, total, span),
        out_shape=(
            pltpu.VMEM(queries.shape, BF16),
            pltpu.VMEM(queries.shape, BF16),
            pltpu.VMEM(key_rows.shape, F32),
            pltpu.VMEM(key_rows.shape, F32),
        ),
        in_specs=[anywhere] * 5,
        out_specs=(pl.BlockSpec(memory_space=pltpu.VMEM),) * 4,
        scratch_shapes=[
            pltpu.VMEM((blocks * tokens, width), BF16),
            pltpu.VMEM((blocks * tokens, width), BF16),
            pltpu.VMEM((blocks, 1, tokens), jnp.int32),
            pltpu.VMEM((stacked, width), BF16),
            pltpu.VMEM((stacked, width), BF16),
            pltpu.VMEM((width, stacked), BF16),
            pltpu.VMEM((width, stacked), BF16),
            pltpu.VMEM((blocks * tokens, width), BF16),
            pltpu.VMEM((width, tokens), BF16),
            pltpu.VMEM((blocks * tokens, stacked), F32),
            pltpu.VMEM((blocks * tokens, stacked), BF16),
            pltpu.VMEM((blocks * tokens, stacked), BF16),
            pltpu.VMEM((blocks * tokens, width), F32),
            pltpu.VMEM((8, stacked), F32),
            pltpu.VMEM((8, stacked), F32),
            pltpu.VMEM((8, stacked), F32),
        ]
        + [block] * 8
        + [sem((3 + 2 * heads,))]
        + [sem((blocks,))] * 6
        + [sem((half,))] * 10,
        compiler_params=pltpu.CompilerParams(
            collective_id=0, has_side_effects=True, vmem_limit_bytes=48 * 1024 * 1024
        ),
    )(*[
        pltpu.with_memory_space_constraint(a, pltpu.HBM)
        for a in (queries, key_rows, value_rows, out_grad, seg_rows)
    ])
    return write_back(results)


def store(*refs):
    count = (len(refs) - 1) // 2
    copies = [pltpu.make_async_copy(refs[i], refs[count + i], refs[-1].at[i]) for i in range(count)]
    for copy in copies:
        copy.start()
    for copy in copies:
        copy.wait()


def write_back(results):
    anywhere = pl.BlockSpec(memory_space=pl.ANY)
    held = [pltpu.with_memory_space_constraint(r, pltpu.VMEM) for r in results]
    return pl.pallas_call(
        store,
        out_shape=tuple(jax.ShapeDtypeStruct(r.shape, r.dtype) for r in results),
        in_specs=[pl.BlockSpec(memory_space=pltpu.VMEM)] * len(results),
        out_specs=(anywhere,) * len(results),
        scratch_shapes=[pltpu.SemaphoreType.DMA((len(results),))],
        compiler_params=pltpu.CompilerParams(vmem_limit_bytes=4 * 1024 * 1024),
    )(*held)


def solution(mesh):
    in_specs = (P(AXES, None), P(AXES, None), P(AXES, None), P(AXES, None), P(AXES))
    out_specs = (P(AXES, None),) * 4
    return jax.shard_map(
        on_device, mesh=mesh, in_specs=in_specs, out_specs=out_specs, check_vma=False
    )
```

```python
import functools
import math

import jax
import jax.numpy as jnp
from jax import lax
from jax.experimental import pallas as pl
from jax.experimental.pallas import tpu as pltpu
from jax.sharding import PartitionSpec as P

MAXDOC = 1536
AXES = ("seq", "grp")
MESH = pl.DeviceIdType.MESH
F32 = jnp.float32
BF16 = jnp.bfloat16
HIDDEN = -1e30
SAME = 8192.0


def dot_nt(a, b):
    return lax.dot_general(a, b, (((1,), (1,)), ((), ())), preferred_element_type=F32)


def dot_nn(a, b):
    return lax.dot_general(a, b, (((1,), (0,)), ((), ())), preferred_element_type=F32)


def kernel(
    groups, total, span,
    q_hbm, k_hbm, v_hbm, g_hbm, seg_hbm,
    o_buf, dq_buf, dk_buf, dv_buf,
    keys, values, segs, qs, gs, qt, gt, hots, marks_t, scores, probs, dscores, value_parts,
    row_max, row_inv, row_dot,
    gk_odd, gv_odd, gk_pair, gv_pair, gk_out, gv_out, gk_in, gv_in, gv_hop,
    local, hop_send, hop_recv,
    k_send, k_recv, s_send, s_recv, v_send, v_recv, kf_send, vf_send,
    gkp_send, gkp_recv, gvp_send, gvp_recv, gk_send, gk_recv, gv_send, gv_recv,
):
    tokens, width = k_hbm.shape
    heads = q_hbm.shape[1] // width
    half = span // 2
    scale = width ** -0.5
    exponent = scale * math.log2(math.e)
    me = lax.axis_index("seq") * groups + lax.axis_index("grp")
    parity = lax.rem(me, 2)
    partner = me + 1 - 2 * parity

    plane = 2 * groups
    hops = plane == 8 and total % plane == 0 and span == 6
    seat = lax.rem(me, plane)
    gives = (seat < 2) if hops else (seat < 0)
    takes = (seat >= 4) & (me >= plane)
    seat_slot = jnp.where(seat >= 6, 0, 1)

    def at(where):
        return (lax.div(where, groups), lax.rem(where, groups))

    def rows(d):
        return pl.ds(pl.multiple_of(d * tokens, tokens), tokens)

    def remote(src, dst, send, recv, where):
        return pltpu.make_async_remote_copy(
            src_ref=src, dst_ref=dst, send_sem=send, recv_sem=recv,
            device_id=at(where), device_id_type=MESH)

    def key_copy(d):
        return remote(keys.at[rows(0)], keys.at[rows(d)], k_send.at[d], k_recv.at[d], me + d)

    def value_copy(d):
        return remote(values.at[rows(0)], values.at[rows(d)], v_send.at[d], v_recv.at[d], me + d)

    def seg_copy(d):
        return remote(segs.at[0], segs.at[d], s_send.at[d], s_recv.at[d], me + d)

    def key_pass_on(j):
        return remote(keys.at[rows(2 * j + 2 * parity)], keys.at[rows(2 * j + 1)],
                      kf_send.at[j], k_recv.at[2 * j + 1], partner)

    def value_pass_on(j):
        return remote(values.at[rows(2 * j + 2 * parity)], values.at[rows(2 * j + 1)],
                      vf_send.at[j], v_recv.at[2 * j + 1], partner)

    def pair_copy(odd, pair, send, recv, j):
        return remote(odd.at[j], pair.at[j], send.at[j], recv.at[j], partner)

    def total_copy(out, into, send, recv, j):
        return remote(out.at[j], into.at[j], send.at[j], recv.at[j], me - 2 * (j + 1))

    def give_copy(j):
        return remote(gv_out.at[j], gv_hop, gv_send.at[j], hop_recv, me + plane - 2 * (j + 1))

    def take_copy():
        return remote(gv_hop, gv_in.at[seat_slot], hop_send, gv_recv.at[seat_slot], me - plane)

    barrier = pltpu.get_barrier_semaphore()
    expected = 0
    for d in [*range(1, span + 1)] + ([plane] if hops else []):
        for way in (d, -d):
            inside = (me + way >= 0) & (me + way < total)
            expected = expected + inside.astype(jnp.int32)

            @pl.when(inside)
            def _():
                pl.semaphore_signal(barrier, inc=1, device_id=at(me + way), device_id_type=MESH)

    key_load = pltpu.make_async_copy(k_hbm, keys.at[pl.ds(0, tokens)], local.at[0])
    seg_load = pltpu.make_async_copy(seg_hbm, segs.at[0], local.at[1])
    value_load = pltpu.make_async_copy(v_hbm, values.at[pl.ds(0, tokens)], local.at[2])
    key_load.start()
    seg_load.start()
    value_load.start()
    loads_q = []
    loads_g = []
    for h in range(heads):
        stacked = pl.ds(h * tokens, tokens)
        head = pl.ds(h * width, width)
        loads_q.append(pltpu.make_async_copy(q_hbm.at[:, head], qs.at[stacked], local.at[3 + h]))
        loads_g.append(pltpu.make_async_copy(g_hbm.at[:, head], gs.at[stacked], local.at[3 + heads + h]))
    for load in loads_q + loads_g:
        load.start()

    for d in range(1, span + 1):
        @pl.when(me < d)
        def _():
            keys[pl.ds(d * tokens, tokens), :] = jnp.zeros((tokens, width), BF16)
            values[pl.ds(d * tokens, tokens), :] = jnp.zeros((tokens, width), BF16)
            hots[pl.ds(d * tokens, tokens), :] = jnp.zeros((tokens, width), BF16)

    key_load.wait()
    seg_load.wait()
    value_load.wait()
    pl.semaphore_wait(barrier, expected)

    for d in range(1, span + 1):
        @pl.when(me + d < total)
        def _():
            seg_copy(d).start()

    @pl.when(parity == 0)
    def _():
        key_pass_on(0).start()

    for d in range(2, span + 1, 2):
        @pl.when(me + d < total)
        def _():
            key_copy(d).start()

    @pl.when(parity == 0)
    def _():
        value_pass_on(0).start()

    def one_hot(d):
        column = jnp.broadcast_to((segs[d] & (width - 1)).astype(F32), (width, tokens)).T
        lane = lax.broadcasted_iota(jnp.int32, (tokens, width), 1).astype(F32)
        return jnp.where(column == lane, 1.0, 0.0)

    for e in range(2, span + 1, 2):
        @pl.when(me + e < total)
        def _():
            value_copy(e).start()

    for load in loads_q + loads_g:
        load.wait()
    for h in range(heads):
        stacked = pl.ds(h * tokens, tokens)
        qt[:, stacked] = qs[stacked, :].T
        gt[:, stacked] = gs[stacked, :].T

    own_hot = one_hot(0)
    hots[pl.ds(0, tokens), :] = own_hot.astype(BF16)
    marks_t[...] = (own_hot * SAME).astype(BF16).T
    row_max[...] = jnp.full(row_max.shape, HIDDEN, F32)

    def score_block(d, diagonal):
        key_block = jnp.concatenate([keys[rows(d), :], hots[rows(d), :]], axis=1)
        for h in range(heads):
            cols = pl.ds(h * tokens, tokens)
            query = jnp.concatenate([qt[:, cols], marks_t[...]], axis=0)
            score = dot_nn(key_block, query) * exponent
            if diagonal:
                key_at = lax.broadcasted_iota(jnp.int32, (tokens, tokens), 0)
                query_at = lax.broadcasted_iota(jnp.int32, (tokens, tokens), 1)
                score = jnp.where(key_at <= query_at, score, HIDDEN)
            scores[rows(d), cols] = score
            top = jnp.max(score.reshape(tokens // 8, 8, tokens), axis=0)
            row_max[:, cols] = jnp.maximum(row_max[:, cols], top)

    score_block(0, True)

    def score_pass(s, carry):
        direct = s <= half
        d = jnp.where(direct, 2 * s, 2 * (s - half) - 1)
        j = s - parity

        @pl.when(me >= d)
        def _():
            key_copy(d).wait_recv()
            seg_copy(d).wait_recv()
            hots[rows(d), :] = one_hot(d).astype(BF16)

        @pl.when(direct & (me >= d) & (j < half))
        def _():
            key_pass_on(j).start()

        score_block(d, False)
        return carry

    lax.fori_loop(1, span + 1, score_pass, 0)
    ones = jnp.ones((16, (span + 1) * tokens), BF16)
    group = 2 * tokens

    def exp_block(h, d, top):
        block = pl.ds(d * tokens, tokens)
        cols = pl.ds(h * tokens, tokens)
        probs[block, cols] = jnp.exp2(scores[block, cols] - top).astype(BF16)

    def normalise(h):
        cols = pl.ds(h * tokens, tokens)
        inverse = 1.0 / dot_nn(ones, probs[:, cols])[0:1, :]
        row_inv[:, cols] = jnp.broadcast_to(inverse, (8, tokens))
        scaled = (gt[:, cols].astype(F32) * inverse).astype(BF16)
        gt[:, cols] = scaled
        gs[cols, :] = scaled.T

    def value_grad(i, d):
        block = pl.ds(d * tokens, tokens)
        cols = pl.ds(i * group, group)
        part = dot_nn(probs[block, cols], gs[cols, :])
        if i > 0:
            part += value_parts[block, :]
        value_parts[block, :] = part

    for i in range(heads // 2):
        e = 2 * i + 2
        if e <= span:
            @pl.when(me >= e)
            def _():
                value_copy(e).wait_recv()

            @pl.when((me >= e) & (e // 2 - parity < half))
            def _():
                value_pass_on(e // 2 - parity).start()

        pair = (2 * i, 2 * i + 1)
        peaks = [jnp.max(row_max[:, pl.ds(h * tokens, tokens)], axis=0, keepdims=True) for h in pair]
        for d in range(span + 1):
            if i > 0:
                value_grad(i - 1, d)
            for h, top in zip(pair, peaks):
                exp_block(h, d, top)
        for h in pair:
            normalise(h)
    for d in range(span + 1):
        value_grad(heads // 2 - 1, d)
    for e in range(heads + 2, span + 1, 2):
        @pl.when(me >= e)
        def _():
            value_copy(e).wait_recv()

        @pl.when((me >= e) & (e // 2 - parity < half))
        def _():
            value_pass_on(e // 2 - parity).start()

    order = [d for m in range(half, 0, -1) for d in (2 * m - 1, 2 * m)]
    order = [5, 3, 6, 1, 4, 2, 0] if span == 6 else order + [0]

    def block_at(s):
        d = order[-1]
        for i in range(len(order) - 1):
            d = jnp.where(s == i, order[i], d)
        return d

    def hand_out(d, part, odd_ref, pair_ref, out_ref, sum_ref, p_send, p_recv, t_send, into, t_recv, hop):
        sum_ref[...] = part
        j = lax.div(jnp.int32(d), 2)
        is_odd = lax.rem(jnp.int32(d), 2) == 1

        @pl.when(is_odd & (me >= d))
        def _():
            odd_ref[j] = sum_ref[...].astype(BF16)
            pair_copy(odd_ref, pair_ref, p_send, p_recv, j).start()

        i = j - parity

        @pl.when(jnp.logical_not(is_odd) & (me >= d) & (i >= 0) & (i < half))
        def _():
            pair_copy(odd_ref, pair_ref, p_send, p_recv, i).wait_recv()
            sum_ref[...] += pair_ref[i].astype(F32)

        @pl.when(jnp.logical_not(is_odd) & (d > 0) & (me >= d))
        def _():
            out_ref[j - 1] = sum_ref[...].astype(BF16)

            @pl.when(gives & hop & (d < span))
            def _():
                give_copy(j - 1).start()

            @pl.when(jnp.logical_not(gives & hop & (d < span)))
            def _():
                total_copy(out_ref, into, t_send, t_recv, j - 1).start()

    def value_hand_out(d):
        hand_out(d, value_parts[rows(d), :], gv_odd, gv_pair, gv_out, dv_buf,
                 gvp_send, gvp_recv, gv_send, gv_in, gv_recv, hops)

    for d in range(span - 1, 0, -2):
        value_hand_out(d)
    for d in range(1, span + 1, 2):
        @pl.when(me >= d)
        def _():
            value_copy(d).wait_recv()

    values_t = values[...].T
    for h in range(heads):
        cols = pl.ds(h * tokens, tokens)
        head = pl.ds(h * width, width)
        attended = (dot_nn(values_t, probs[:, cols]) * row_inv[0:1, cols]).astype(BF16)
        dot = jnp.sum(attended.astype(F32) * gt[:, cols].astype(F32), axis=0, keepdims=True)
        row_dot[:, cols] = jnp.broadcast_to(dot, (8, tokens))
        o_buf[:, head] = attended.T
        if h == heads // 2 - 1:
            for d in range(span, -1, -2):
                value_hand_out(d)

    def key_grad_pass(s, carry):
        d = block_at(s)
        if hops:
            @pl.when((s == span) & takes)
            def _():
                give_copy(0).wait_recv()
                take_copy().start()

        value_block = values[rows(d), :]
        for h in range(heads):
            cols = pl.ds(h * tokens, tokens)
            dprob = dot_nn(value_block, gt[:, cols])
            prob = probs[rows(d), cols].astype(F32)
            dscores[rows(d), cols] = (prob * (dprob - row_dot[0:1, cols])).astype(BF16)
        part = dot_nn(dscores[rows(d), :], qs[...]) * scale
        hand_out(d, part, gk_odd, gk_pair, gk_out, dk_buf, gkp_send, gkp_recv, gk_send, gk_in, gk_recv, False)
        return carry

    lax.fori_loop(0, span + 1, key_grad_pass, 0)
    keys_t = keys[...].T
    for h in range(heads):
        cols = pl.ds(h * tokens, tokens)
        grad = (dot_nn(keys_t, dscores[:, cols]) * scale).astype(BF16)
        dq_buf[:, pl.ds(h * width, width)] = grad.T

    for j in range(half - 1, -1, -1):
        @pl.when(me + 2 * (j + 1) < total)
        def _():
            total_copy(gv_out, gv_in, gv_send, gv_recv, j).wait_recv()
            dv_buf[...] += gv_in[j].astype(F32)

    for j in range(half - 1, -1, -1):
        @pl.when(me + 2 * (j + 1) < total)
        def _():
            total_copy(gk_out, gk_in, gk_send, gk_recv, j).wait_recv()
            dk_buf[...] += gk_in[j].astype(F32)


    if hops:
        @pl.when(takes)
        def _():
            take_copy().wait_send()
    for d in range(1, span + 1):
        @pl.when(me + d < total)
        def _():
            seg_copy(d).wait_send()
            if d % 2 == 0:
                key_copy(d).wait_send()
                value_copy(d).wait_send()
    for j in range(half):
        @pl.when(me >= 2 * j + 2 * parity)
        def _():
            key_pass_on(j).wait_send()
            value_pass_on(j).wait_send()

        @pl.when(me >= 2 * j + 1)
        def _():
            pair_copy(gv_odd, gv_pair, gvp_send, gvp_recv, j).wait_send()
            pair_copy(gk_odd, gk_pair, gkp_send, gkp_recv, j).wait_send()

        @pl.when(me >= 2 * j + 2)
        def _():
            total_copy(gv_out, gv_in, gv_send, gv_recv, j).wait_send()
            total_copy(gk_out, gk_in, gk_send, gk_recv, j).wait_send()


def on_device(queries, key_rows, value_rows, out_grad, segment):
    tokens, width = key_rows.shape
    heads = queries.shape[1] // width
    groups = lax.axis_size("grp")
    total = groups * lax.axis_size("seq")
    span = -(-MAXDOC // tokens)
    span += span % 2
    blocks = span + 1
    half = span // 2
    stacked = heads * tokens
    seg_rows = segment.reshape(1, tokens)
    anywhere = pl.BlockSpec(memory_space=pl.ANY)
    sem = pltpu.SemaphoreType.DMA
    block = pltpu.VMEM((half, tokens, width), BF16)
    results = pl.pallas_call(
        functools.partial(kernel, groups, total, span),
        out_shape=(
            pltpu.VMEM(queries.shape, BF16),
            pltpu.VMEM(queries.shape, BF16),
            pltpu.VMEM(key_rows.shape, F32),
            pltpu.VMEM(key_rows.shape, F32),
        ),
        in_specs=[anywhere] * 5,
        out_specs=(pl.BlockSpec(memory_space=pltpu.VMEM),) * 4,
        scratch_shapes=[
            pltpu.VMEM((blocks * tokens, width), BF16),
            pltpu.VMEM((blocks * tokens, width), BF16),
            pltpu.VMEM((blocks, 1, tokens), jnp.int32),
            pltpu.VMEM((stacked, width), BF16),
            pltpu.VMEM((stacked, width), BF16),
            pltpu.VMEM((width, stacked), BF16),
            pltpu.VMEM((width, stacked), BF16),
            pltpu.VMEM((blocks * tokens, width), BF16),
            pltpu.VMEM((width, tokens), BF16),
            pltpu.VMEM((blocks * tokens, stacked), F32),
            pltpu.VMEM((blocks * tokens, stacked), BF16),
            pltpu.VMEM((blocks * tokens, stacked), BF16),
            pltpu.VMEM((blocks * tokens, width), F32),
            pltpu.VMEM((8, stacked), F32),
            pltpu.VMEM((8, stacked), F32),
            pltpu.VMEM((8, stacked), F32),
        ]
        + [block] * 8
        + [pltpu.VMEM((tokens, width), BF16)]
        + [sem((3 + 2 * heads,)), sem, sem]
        + [sem((blocks,))] * 6
        + [sem((half,))] * 10,
        compiler_params=pltpu.CompilerParams(
            collective_id=0, has_side_effects=True, vmem_limit_bytes=48 * 1024 * 1024
        ),
    )(*[
        pltpu.with_memory_space_constraint(a, pltpu.HBM)
        for a in (queries, key_rows, value_rows, out_grad, seg_rows)
    ])
    return write_back(results)


def store(*refs):
    count = (len(refs) - 1) // 2
    copies = [pltpu.make_async_copy(refs[i], refs[count + i], refs[-1].at[i]) for i in range(count)]
    for copy in copies:
        copy.start()
    for copy in copies:
        copy.wait()


def write_back(results):
    anywhere = pl.BlockSpec(memory_space=pl.ANY)
    held = [pltpu.with_memory_space_constraint(r, pltpu.VMEM) for r in results]
    return pl.pallas_call(
        store,
        out_shape=tuple(jax.ShapeDtypeStruct(r.shape, r.dtype) for r in results),
        in_specs=[pl.BlockSpec(memory_space=pltpu.VMEM)] * len(results),
        out_specs=(anywhere,) * len(results),
        scratch_shapes=[pltpu.SemaphoreType.DMA((len(results),))],
        compiler_params=pltpu.CompilerParams(vmem_limit_bytes=4 * 1024 * 1024),
    )(*held)


def solution(mesh):
    in_specs = (P(AXES, None), P(AXES, None), P(AXES, None), P(AXES, None), P(AXES))
    out_specs = (P(AXES, None),) * 4
    return jax.shard_map(
        on_device, mesh=mesh, in_specs=in_specs, out_specs=out_specs, check_vma=False
    )
```

```python
import functools
import math

import jax
import jax.numpy as jnp
from jax import lax
from jax.experimental import pallas as pl
from jax.experimental.pallas import tpu as pltpu
from jax.sharding import PartitionSpec as P

MAXDOC = 1536
AXES = ("seq", "grp")
MESH = pl.DeviceIdType.MESH
F32 = jnp.float32
BF16 = jnp.bfloat16
HIDDEN = -1e30
SAME = 8192.0


def dot_nt(a, b):
    return lax.dot_general(a, b, (((1,), (1,)), ((), ())), preferred_element_type=F32)


def dot_nn(a, b):
    return lax.dot_general(a, b, (((1,), (0,)), ((), ())), preferred_element_type=F32)


def kernel(
    groups, total, span,
    q_hbm, k_hbm, v_hbm, g_hbm, seg_hbm,
    o_buf, dq_buf, dk_buf, dv_buf,
    keys, values, segs, qs, gs, qt, gt, hots, marks_t, scores, probs, dscores, value_parts,
    row_max, row_inv, row_dot,
    gk_odd, gv_odd, gk_pair, gv_pair, gk_out, gv_out, gk_in, gv_in, gv_hop,
    local, hop_send, hop_recv,
    k_send, k_recv, s_send, s_recv, v_send, v_recv, kf_send, vf_send,
    gkp_send, gkp_recv, gvp_send, gvp_recv, gk_send, gk_recv, gv_send, gv_recv,
):
    tokens, width = k_hbm.shape
    heads = q_hbm.shape[1] // width
    half = span // 2
    scale = width ** -0.5
    exponent = scale * math.log2(math.e)
    me = lax.axis_index("seq") * groups + lax.axis_index("grp")
    parity = lax.rem(me, 2)
    partner = me + 1 - 2 * parity

    plane = 2 * groups
    hops = plane == 8 and total % plane == 0 and span == 6
    seat = lax.rem(me, plane)
    gives = (seat < 2) if hops else (seat < 0)
    takes = (seat >= 4) & (me >= plane)
    seat_slot = jnp.where(seat >= 6, 0, 1)

    def at(where):
        return (lax.div(where, groups), lax.rem(where, groups))

    def rows(d):
        return pl.ds(pl.multiple_of(d * tokens, tokens), tokens)

    def remote(src, dst, send, recv, where):
        return pltpu.make_async_remote_copy(
            src_ref=src, dst_ref=dst, send_sem=send, recv_sem=recv,
            device_id=at(where), device_id_type=MESH)

    def key_copy(d):
        return remote(keys.at[rows(0)], keys.at[rows(d)], k_send.at[d], k_recv.at[d], me + d)

    def value_copy(d):
        return remote(values.at[rows(0)], values.at[rows(d)], v_send.at[d], v_recv.at[d], me + d)

    def seg_copy(d):
        return remote(segs.at[0], segs.at[d], s_send.at[d], s_recv.at[d], me + d)

    def key_pass_on(j):
        return remote(keys.at[rows(2 * j + 2 * parity)], keys.at[rows(2 * j + 1)],
                      kf_send.at[j], k_recv.at[2 * j + 1], partner)

    def value_pass_on(j):
        return remote(values.at[rows(2 * j + 2 * parity)], values.at[rows(2 * j + 1)],
                      vf_send.at[j], v_recv.at[2 * j + 1], partner)

    def pair_copy(odd, pair, send, recv, j):
        return remote(odd.at[j], pair.at[j], send.at[j], recv.at[j], partner)

    def total_copy(out, into, send, recv, j):
        return remote(out.at[j], into.at[j], send.at[j], recv.at[j], me - 2 * (j + 1))

    def give_copy(j):
        return remote(gv_out.at[j], gv_hop, gv_send.at[j], hop_recv, me + plane - 2 * (j + 1))

    def take_copy():
        return remote(gv_hop, gv_in.at[seat_slot], hop_send, gv_recv.at[seat_slot], me - plane)

    barrier = pltpu.get_barrier_semaphore()
    expected = 0
    for d in [*range(1, span + 1)] + ([plane] if hops else []):
        for way in (d, -d):
            inside = (me + way >= 0) & (me + way < total)
            expected = expected + inside.astype(jnp.int32)

            @pl.when(inside)
            def _():
                pl.semaphore_signal(barrier, inc=1, device_id=at(me + way), device_id_type=MESH)

    key_load = pltpu.make_async_copy(k_hbm, keys.at[pl.ds(0, tokens)], local.at[0])
    seg_load = pltpu.make_async_copy(seg_hbm, segs.at[0], local.at[1])
    value_load = pltpu.make_async_copy(v_hbm, values.at[pl.ds(0, tokens)], local.at[2])
    key_load.start()
    seg_load.start()
    value_load.start()
    loads_q = []
    loads_g = []
    for h in range(heads):
        stacked = pl.ds(h * tokens, tokens)
        head = pl.ds(h * width, width)
        loads_q.append(pltpu.make_async_copy(q_hbm.at[:, head], qs.at[stacked], local.at[3 + h]))
        loads_g.append(pltpu.make_async_copy(g_hbm.at[:, head], gs.at[stacked], local.at[3 + heads + h]))
    for load in loads_q + loads_g:
        load.start()

    for d in range(1, span + 1):
        @pl.when(me < d)
        def _():
            keys[pl.ds(d * tokens, tokens), :] = jnp.zeros((tokens, width), BF16)
            values[pl.ds(d * tokens, tokens), :] = jnp.zeros((tokens, width), BF16)
            hots[pl.ds(d * tokens, tokens), :] = jnp.zeros((tokens, width), BF16)

    key_load.wait()
    seg_load.wait()
    value_load.wait()
    pl.semaphore_wait(barrier, expected)

    for d in range(1, span + 1):
        @pl.when(me + d < total)
        def _():
            seg_copy(d).start()

    @pl.when(parity == 0)
    def _():
        key_pass_on(0).start()

    for d in range(2, span + 1, 2):
        @pl.when(me + d < total)
        def _():
            key_copy(d).start()

    @pl.when(parity == 0)
    def _():
        value_pass_on(0).start()

    def one_hot(d):
        column = jnp.broadcast_to((segs[d] & (width - 1)).astype(F32), (width, tokens)).T
        lane = lax.broadcasted_iota(jnp.int32, (tokens, width), 1).astype(F32)
        return jnp.where(column == lane, 1.0, 0.0)

    for e in range(2, span + 1, 2):
        @pl.when(me + e < total)
        def _():
            value_copy(e).start()

    for load in loads_q + loads_g:
        load.wait()
    for h in range(heads):
        stacked = pl.ds(h * tokens, tokens)
        qt[:, stacked] = qs[stacked, :].T
        gt[:, stacked] = gs[stacked, :].T

    own_hot = one_hot(0)
    hots[pl.ds(0, tokens), :] = own_hot.astype(BF16)
    marks_t[...] = (own_hot * SAME).astype(BF16).T
    row_max[...] = jnp.full(row_max.shape, HIDDEN, F32)

    def score_block(d, diagonal):
        key_block = jnp.concatenate([keys[rows(d), :], hots[rows(d), :]], axis=1)
        for h in range(heads):
            cols = pl.ds(h * tokens, tokens)
            query = jnp.concatenate([qt[:, cols], marks_t[...]], axis=0)
            score = dot_nn(key_block, query) * exponent
            if diagonal:
                key_at = lax.broadcasted_iota(jnp.int32, (tokens, tokens), 0)
                query_at = lax.broadcasted_iota(jnp.int32, (tokens, tokens), 1)
                score = jnp.where(key_at <= query_at, score, HIDDEN)
            scores[rows(d), cols] = score
            top = jnp.max(score.reshape(tokens // 8, 8, tokens), axis=0)
            row_max[:, cols] = jnp.maximum(row_max[:, cols], top)

    score_block(0, True)

    def score_pass(s, carry):
        direct = s <= half
        d = jnp.where(direct, 2 * s, 2 * (s - half) - 1)
        j = s - parity

        @pl.when(me >= d)
        def _():
            key_copy(d).wait_recv()
            seg_copy(d).wait_recv()
            hots[rows(d), :] = one_hot(d).astype(BF16)

        @pl.when(direct & (me >= d) & (j < half))
        def _():
            key_pass_on(j).start()

        score_block(d, False)
        return carry

    lax.fori_loop(1, span + 1, score_pass, 0)
    ones = jnp.ones((16, (span + 1) * tokens), BF16)
    group = 2 * tokens

    def exp_block(h, d, top):
        block = pl.ds(d * tokens, tokens)
        cols = pl.ds(h * tokens, tokens)
        probs[block, cols] = jnp.exp2(scores[block, cols] - top).astype(BF16)

    def normalise(h):
        cols = pl.ds(h * tokens, tokens)
        inverse = 1.0 / dot_nn(ones, probs[:, cols])[0:1, :]
        row_inv[:, cols] = jnp.broadcast_to(inverse, (8, tokens))
        scaled = (gt[:, cols].astype(F32) * inverse).astype(BF16)
        gt[:, cols] = scaled
        gs[cols, :] = scaled.T

    def value_grad(i, d):
        block = pl.ds(d * tokens, tokens)
        cols = pl.ds(i * group, group)
        part = dot_nn(probs[block, cols], gs[cols, :])
        if i > 0:
            part += value_parts[block, :]
        value_parts[block, :] = part

    for i in range(heads // 2):
        e = 2 * i + 2
        if e <= span:
            @pl.when(me >= e)
            def _():
                value_copy(e).wait_recv()

            @pl.when((me >= e) & (e // 2 - parity < half))
            def _():
                value_pass_on(e // 2 - parity).start()

        pair = (2 * i, 2 * i + 1)
        peaks = [jnp.max(row_max[:, pl.ds(h * tokens, tokens)], axis=0, keepdims=True) for h in pair]
        for d in range(span + 1):
            if i > 0:
                value_grad(i - 1, d)
            for h, top in zip(pair, peaks):
                exp_block(h, d, top)
        for h in pair:
            normalise(h)
    for d in range(span + 1):
        value_grad(heads // 2 - 1, d)
    for e in range(heads + 2, span + 1, 2):
        @pl.when(me >= e)
        def _():
            value_copy(e).wait_recv()

        @pl.when((me >= e) & (e // 2 - parity < half))
        def _():
            value_pass_on(e // 2 - parity).start()

    order = [d for m in range(half, 0, -1) for d in (2 * m - 1, 2 * m)]
    order = [5, 6, 3, 4, 1, 2, 0] if span == 6 else order + [0]

    def block_at(s):
        d = order[-1]
        for i in range(len(order) - 1):
            d = jnp.where(s == i, order[i], d)
        return d

    def hand_out(d, part, odd_ref, pair_ref, out_ref, sum_ref, p_send, p_recv, t_send, into, t_recv, hop):
        sum_ref[...] = part
        j = lax.div(jnp.int32(d), 2)
        is_odd = lax.rem(jnp.int32(d), 2) == 1

        @pl.when(is_odd & (me >= d))
        def _():
            odd_ref[j] = sum_ref[...].astype(BF16)
            pair_copy(odd_ref, pair_ref, p_send, p_recv, j).start()

        i = j - parity

        @pl.when(jnp.logical_not(is_odd) & (me >= d) & (i >= 0) & (i < half))
        def _():
            pair_copy(odd_ref, pair_ref, p_send, p_recv, i).wait_recv()
            sum_ref[...] += pair_ref[i].astype(F32)

        @pl.when(jnp.logical_not(is_odd) & (d > 0) & (me >= d))
        def _():
            out_ref[j - 1] = sum_ref[...].astype(BF16)

            @pl.when(gives & hop & (d < span))
            def _():
                give_copy(j - 1).start()

            @pl.when(jnp.logical_not(gives & hop & (d < span)))
            def _():
                total_copy(out_ref, into, t_send, t_recv, j - 1).start()

    def value_hand_out(d):
        hand_out(d, value_parts[rows(d), :], gv_odd, gv_pair, gv_out, dv_buf,
                 gvp_send, gvp_recv, gv_send, gv_in, gv_recv, hops)

    for d in range(span - 1, 0, -2):
        value_hand_out(d)
    for d in range(1, span + 1, 2):
        @pl.when(me >= d)
        def _():
            value_copy(d).wait_recv()

    values_t = values[...].T
    for h in range(heads):
        cols = pl.ds(h * tokens, tokens)
        head = pl.ds(h * width, width)
        attended = (dot_nn(values_t, probs[:, cols]) * row_inv[0:1, cols]).astype(BF16)
        dot = jnp.sum(attended.astype(F32) * gt[:, cols].astype(F32), axis=0, keepdims=True)
        row_dot[:, cols] = jnp.broadcast_to(dot, (8, tokens))
        o_buf[:, head] = attended.T
        if h == heads // 2 - 1:
            for d in range(span, -1, -2):
                value_hand_out(d)

    def key_grad_pass(s, carry):
        d = block_at(s)
        if hops:
            @pl.when((s == span) & takes)
            def _():
                give_copy(0).wait_recv()
                take_copy().start()

        value_block = values[rows(d), :]
        for h in range(heads):
            cols = pl.ds(h * tokens, tokens)
            dprob = dot_nn(value_block, gt[:, cols])
            prob = probs[rows(d), cols].astype(F32)
            dscores[rows(d), cols] = (prob * (dprob - row_dot[0:1, cols])).astype(BF16)
        part = dot_nn(dscores[rows(d), :], qs[...]) * scale
        hand_out(d, part, gk_odd, gk_pair, gk_out, dk_buf, gkp_send, gkp_recv, gk_send, gk_in, gk_recv, False)
        return carry

    lax.fori_loop(0, span + 1, key_grad_pass, 0)
    keys_t = keys[...].T
    for h in range(heads):
        cols = pl.ds(h * tokens, tokens)
        grad = (dot_nn(keys_t, dscores[:, cols]) * scale).astype(BF16)
        dq_buf[:, pl.ds(h * width, width)] = grad.T

    for j in range(half - 1, -1, -1):
        @pl.when(me + 2 * (j + 1) < total)
        def _():
            total_copy(gv_out, gv_in, gv_send, gv_recv, j).wait_recv()
            dv_buf[...] += gv_in[j].astype(F32)

    for j in range(half - 1, -1, -1):
        @pl.when(me + 2 * (j + 1) < total)
        def _():
            total_copy(gk_out, gk_in, gk_send, gk_recv, j).wait_recv()
            dk_buf[...] += gk_in[j].astype(F32)


    if hops:
        @pl.when(takes)
        def _():
            take_copy().wait_send()
    for d in range(1, span + 1):
        @pl.when(me + d < total)
        def _():
            seg_copy(d).wait_send()
            if d % 2 == 0:
                key_copy(d).wait_send()
                value_copy(d).wait_send()
    for j in range(half):
        @pl.when(me >= 2 * j + 2 * parity)
        def _():
            key_pass_on(j).wait_send()
            value_pass_on(j).wait_send()

        @pl.when(me >= 2 * j + 1)
        def _():
            pair_copy(gv_odd, gv_pair, gvp_send, gvp_recv, j).wait_send()
            pair_copy(gk_odd, gk_pair, gkp_send, gkp_recv, j).wait_send()

        @pl.when(me >= 2 * j + 2)
        def _():
            total_copy(gv_out, gv_in, gv_send, gv_recv, j).wait_send()
            total_copy(gk_out, gk_in, gk_send, gk_recv, j).wait_send()


def on_device(queries, key_rows, value_rows, out_grad, segment):
    tokens, width = key_rows.shape
    heads = queries.shape[1] // width
    groups = lax.axis_size("grp")
    total = groups * lax.axis_size("seq")
    span = -(-MAXDOC // tokens)
    span += span % 2
    blocks = span + 1
    half = span // 2
    stacked = heads * tokens
    seg_rows = segment.reshape(1, tokens)
    anywhere = pl.BlockSpec(memory_space=pl.ANY)
    sem = pltpu.SemaphoreType.DMA
    block = pltpu.VMEM((half, tokens, width), BF16)
    results = pl.pallas_call(
        functools.partial(kernel, groups, total, span),
        out_shape=(
            pltpu.VMEM(queries.shape, BF16),
            pltpu.VMEM(queries.shape, BF16),
            pltpu.VMEM(key_rows.shape, F32),
            pltpu.VMEM(key_rows.shape, F32),
        ),
        in_specs=[anywhere] * 5,
        out_specs=(pl.BlockSpec(memory_space=pltpu.VMEM),) * 4,
        scratch_shapes=[
            pltpu.VMEM((blocks * tokens, width), BF16),
            pltpu.VMEM((blocks * tokens, width), BF16),
            pltpu.VMEM((blocks, 1, tokens), jnp.int32),
            pltpu.VMEM((stacked, width), BF16),
            pltpu.VMEM((stacked, width), BF16),
            pltpu.VMEM((width, stacked), BF16),
            pltpu.VMEM((width, stacked), BF16),
            pltpu.VMEM((blocks * tokens, width), BF16),
            pltpu.VMEM((width, tokens), BF16),
            pltpu.VMEM((blocks * tokens, stacked), F32),
            pltpu.VMEM((blocks * tokens, stacked), BF16),
            pltpu.VMEM((blocks * tokens, stacked), BF16),
            pltpu.VMEM((blocks * tokens, width), F32),
            pltpu.VMEM((8, stacked), F32),
            pltpu.VMEM((8, stacked), F32),
            pltpu.VMEM((8, stacked), F32),
        ]
        + [block] * 8
        + [pltpu.VMEM((tokens, width), BF16)]
        + [sem((3 + 2 * heads,)), sem, sem]
        + [sem((blocks,))] * 6
        + [sem((half,))] * 10,
        compiler_params=pltpu.CompilerParams(
            collective_id=0, has_side_effects=True, vmem_limit_bytes=48 * 1024 * 1024
        ),
    )(*[
        pltpu.with_memory_space_constraint(a, pltpu.HBM)
        for a in (queries, key_rows, value_rows, out_grad, seg_rows)
    ])
    return write_back(results)


def store(*refs):
    count = (len(refs) - 1) // 2
    copies = [pltpu.make_async_copy(refs[i], refs[count + i], refs[-1].at[i]) for i in range(count)]
    for copy in copies:
        copy.start()
    for copy in copies:
        copy.wait()


def write_back(results):
    anywhere = pl.BlockSpec(memory_space=pl.ANY)
    held = [pltpu.with_memory_space_constraint(r, pltpu.VMEM) for r in results]
    return pl.pallas_call(
        store,
        out_shape=tuple(jax.ShapeDtypeStruct(r.shape, r.dtype) for r in results),
        in_specs=[pl.BlockSpec(memory_space=pltpu.VMEM)] * len(results),
        out_specs=(anywhere,) * len(results),
        scratch_shapes=[pltpu.SemaphoreType.DMA((len(results),))],
        compiler_params=pltpu.CompilerParams(vmem_limit_bytes=4 * 1024 * 1024),
    )(*held)


def solution(mesh):
    in_specs = (P(AXES, None), P(AXES, None), P(AXES, None), P(AXES, None), P(AXES))
    out_specs = (P(AXES, None),) * 4
    return jax.shard_map(
        on_device, mesh=mesh, in_specs=in_specs, out_specs=out_specs, check_vma=False
    )
```

```python
import functools
import math

import jax
import jax.numpy as jnp
from jax import lax
from jax.experimental import pallas as pl
from jax.experimental.pallas import tpu as pltpu
from jax.sharding import PartitionSpec as P

MAXDOC = 1536
AXES = ("seq", "grp")
MESH = pl.DeviceIdType.MESH
F32 = jnp.float32
BF16 = jnp.bfloat16
HIDDEN = -1e30
SAME = 8192.0


def dot_nt(a, b):
    return lax.dot_general(a, b, (((1,), (1,)), ((), ())), preferred_element_type=F32)


def dot_nn(a, b):
    return lax.dot_general(a, b, (((1,), (0,)), ((), ())), preferred_element_type=F32)


def kernel(
    groups, total, span,
    q_hbm, k_hbm, v_hbm, g_hbm, seg_hbm,
    o_buf, dq_buf, dk_buf, dv_buf,
    keys, values, segs, qs, gs, qt, gt, hots, marks_t, scores, probs, dscores, value_parts,
    row_max, row_inv, row_dot,
    gk_odd, gv_odd, gk_pair, gv_pair, gk_out, gv_out, gk_in, gv_in, gv_hop,
    local, hop_send, hop_recv,
    k_send, k_recv, s_send, s_recv, v_send, v_recv, kf_send, vf_send,
    gkp_send, gkp_recv, gvp_send, gvp_recv, gk_send, gk_recv, gv_send, gv_recv,
):
    tokens, width = k_hbm.shape
    heads = q_hbm.shape[1] // width
    half = span // 2
    scale = width ** -0.5
    exponent = scale * math.log2(math.e)
    me = lax.axis_index("seq") * groups + lax.axis_index("grp")
    parity = lax.rem(me, 2)
    partner = me + 1 - 2 * parity

    plane = 2 * groups
    hops = plane == 8 and total % plane == 0 and span == 6
    seat = lax.rem(me, plane)
    gives = (seat < 2) if hops else (seat < 0)
    takes = (seat >= 4) & (me >= plane)
    seat_slot = jnp.where(seat >= 6, 0, 1)

    def at(where):
        return (lax.div(where, groups), lax.rem(where, groups))

    def rows(d):
        return pl.ds(pl.multiple_of(d * tokens, tokens), tokens)

    def remote(src, dst, send, recv, where):
        return pltpu.make_async_remote_copy(
            src_ref=src, dst_ref=dst, send_sem=send, recv_sem=recv,
            device_id=at(where), device_id_type=MESH)

    def key_copy(d):
        return remote(keys.at[rows(0)], keys.at[rows(d)], k_send.at[d], k_recv.at[d], me + d)

    def value_copy(d):
        return remote(values.at[rows(0)], values.at[rows(d)], v_send.at[d], v_recv.at[d], me + d)

    def seg_copy(d):
        return remote(segs.at[0], segs.at[d], s_send.at[d], s_recv.at[d], me + d)

    def key_pass_on(j):
        return remote(keys.at[rows(2 * j + 2 * parity)], keys.at[rows(2 * j + 1)],
                      kf_send.at[j], k_recv.at[2 * j + 1], partner)

    def value_pass_on(j):
        return remote(values.at[rows(2 * j + 2 * parity)], values.at[rows(2 * j + 1)],
                      vf_send.at[j], v_recv.at[2 * j + 1], partner)

    def pair_copy(odd, pair, send, recv, j):
        return remote(odd.at[j], pair.at[j], send.at[j], recv.at[j], partner)

    def total_copy(out, into, send, recv, j):
        return remote(out.at[j], into.at[j], send.at[j], recv.at[j], me - 2 * (j + 1))

    def give_copy(j):
        return remote(gv_out.at[j], gv_hop, gv_send.at[j], hop_recv, me + plane - 2 * (j + 1))

    def take_copy():
        return remote(gv_hop, gv_in.at[seat_slot], hop_send, gv_recv.at[seat_slot], me - plane)

    barrier = pltpu.get_barrier_semaphore()
    expected = 0
    for d in [*range(1, span + 1)] + ([plane] if hops else []):
        for way in (d, -d):
            inside = (me + way >= 0) & (me + way < total)
            expected = expected + inside.astype(jnp.int32)

            @pl.when(inside)
            def _():
                pl.semaphore_signal(barrier, inc=1, device_id=at(me + way), device_id_type=MESH)

    key_load = pltpu.make_async_copy(k_hbm, keys.at[pl.ds(0, tokens)], local.at[0])
    seg_load = pltpu.make_async_copy(seg_hbm, segs.at[0], local.at[1])
    value_load = pltpu.make_async_copy(v_hbm, values.at[pl.ds(0, tokens)], local.at[2])
    key_load.start()
    seg_load.start()
    value_load.start()
    loads_q = []
    loads_g = []
    for h in range(heads):
        stacked = pl.ds(h * tokens, tokens)
        head = pl.ds(h * width, width)
        loads_q.append(pltpu.make_async_copy(q_hbm.at[:, head], qs.at[stacked], local.at[3 + h]))
        loads_g.append(pltpu.make_async_copy(g_hbm.at[:, head], gs.at[stacked], local.at[3 + heads + h]))
    for load in loads_q + loads_g:
        load.start()

    for d in range(1, span + 1):
        @pl.when(me < d)
        def _():
            keys[pl.ds(d * tokens, tokens), :] = jnp.zeros((tokens, width), BF16)
            values[pl.ds(d * tokens, tokens), :] = jnp.zeros((tokens, width), BF16)
            hots[pl.ds(d * tokens, tokens), :] = jnp.zeros((tokens, width), BF16)

    key_load.wait()
    seg_load.wait()
    value_load.wait()
    pl.semaphore_wait(barrier, expected)

    for d in range(1, span + 1):
        @pl.when(me + d < total)
        def _():
            seg_copy(d).start()

    @pl.when(parity == 0)
    def _():
        key_pass_on(0).start()

    for d in range(2, span + 1, 2):
        @pl.when(me + d < total)
        def _():
            key_copy(d).start()

    @pl.when(parity == 0)
    def _():
        value_pass_on(0).start()

    def one_hot(d):
        column = jnp.broadcast_to((segs[d] & (width - 1)).astype(F32), (width, tokens)).T
        lane = lax.broadcasted_iota(jnp.int32, (tokens, width), 1).astype(F32)
        return jnp.where(column == lane, 1.0, 0.0)

    for e in range(2, span + 1, 2):
        @pl.when(me + e < total)
        def _():
            value_copy(e).start()

    for load in loads_q + loads_g:
        load.wait()
    for h in range(heads):
        stacked = pl.ds(h * tokens, tokens)
        qt[:, stacked] = qs[stacked, :].T
        gt[:, stacked] = gs[stacked, :].T

    own_hot = one_hot(0)
    hots[pl.ds(0, tokens), :] = own_hot.astype(BF16)
    marks_t[...] = (own_hot * SAME).astype(BF16).T
    row_max[...] = jnp.full(row_max.shape, HIDDEN, F32)

    def score_block(d, diagonal):
        key_block = jnp.concatenate([keys[rows(d), :], hots[rows(d), :]], axis=1)
        for h in range(heads):
            cols = pl.ds(h * tokens, tokens)
            query = jnp.concatenate([qt[:, cols], marks_t[...]], axis=0)
            score = dot_nn(key_block, query) * exponent
            if diagonal:
                key_at = lax.broadcasted_iota(jnp.int32, (tokens, tokens), 0)
                query_at = lax.broadcasted_iota(jnp.int32, (tokens, tokens), 1)
                score = jnp.where(key_at <= query_at, score, HIDDEN)
            scores[rows(d), cols] = score
            top = jnp.max(score.reshape(tokens // 8, 8, tokens), axis=0)
            row_max[:, cols] = jnp.maximum(row_max[:, cols], top)

    score_block(0, True)

    def score_pass(s, carry):
        direct = s <= half
        d = jnp.where(direct, 2 * s, 2 * (s - half) - 1)
        j = s - parity

        @pl.when(me >= d)
        def _():
            key_copy(d).wait_recv()
            seg_copy(d).wait_recv()
            hots[rows(d), :] = one_hot(d).astype(BF16)

        @pl.when(direct & (me >= d) & (j < half))
        def _():
            key_pass_on(j).start()

        score_block(d, False)
        return carry

    lax.fori_loop(1, span + 1, score_pass, 0)
    ones = jnp.ones((16, (span + 1) * tokens), BF16)
    group = 2 * tokens

    def exp_block(h, d, top):
        block = pl.ds(d * tokens, tokens)
        cols = pl.ds(h * tokens, tokens)
        probs[block, cols] = jnp.exp2(scores[block, cols] - top).astype(BF16)

    def normalise(h):
        cols = pl.ds(h * tokens, tokens)
        inverse = 1.0 / dot_nn(ones, probs[:, cols])[0:1, :]
        row_inv[:, cols] = jnp.broadcast_to(inverse, (8, tokens))
        scaled = (gt[:, cols].astype(F32) * inverse).astype(BF16)
        gt[:, cols] = scaled
        gs[cols, :] = scaled.T

    def value_grad(i, d):
        block = pl.ds(d * tokens, tokens)
        cols = pl.ds(i * group, group)
        part = dot_nn(probs[block, cols], gs[cols, :])
        if i > 0:
            part += value_parts[block, :]
        value_parts[block, :] = part

    for i in range(heads // 2):
        e = 2 * i + 2
        if e <= span:
            @pl.when(me >= e)
            def _():
                value_copy(e).wait_recv()

            @pl.when((me >= e) & (e // 2 - parity < half))
            def _():
                value_pass_on(e // 2 - parity).start()

        pair = (2 * i, 2 * i + 1)
        peaks = [jnp.max(row_max[:, pl.ds(h * tokens, tokens)], axis=0, keepdims=True) for h in pair]
        for d in range(span + 1):
            if i > 0:
                value_grad(i - 1, d)
            for h, top in zip(pair, peaks):
                exp_block(h, d, top)
        for h in pair:
            normalise(h)
    for d in range(span + 1):
        value_grad(heads // 2 - 1, d)
    for e in range(heads + 2, span + 1, 2):
        @pl.when(me >= e)
        def _():
            value_copy(e).wait_recv()

        @pl.when((me >= e) & (e // 2 - parity < half))
        def _():
            value_pass_on(e // 2 - parity).start()

    order = [d for m in range(half, 0, -1) for d in (2 * m - 1, 2 * m)]
    order = [5, 6, 3, 4, 1, 2, 0] if span == 6 else order + [0]

    def block_at(s):
        d = order[-1]
        for i in range(len(order) - 1):
            d = jnp.where(s == i, order[i], d)
        return d

    def hand_out(d, part, odd_ref, pair_ref, out_ref, sum_ref, p_send, p_recv, t_send, into, t_recv, hop):
        sum_ref[...] = part
        j = lax.div(jnp.int32(d), 2)
        is_odd = lax.rem(jnp.int32(d), 2) == 1

        @pl.when(is_odd & (me >= d))
        def _():
            odd_ref[j] = sum_ref[...].astype(BF16)
            pair_copy(odd_ref, pair_ref, p_send, p_recv, j).start()

        i = j - parity

        @pl.when(jnp.logical_not(is_odd) & (me >= d) & (i >= 0) & (i < half))
        def _():
            pair_copy(odd_ref, pair_ref, p_send, p_recv, i).wait_recv()
            sum_ref[...] += pair_ref[i].astype(F32)

        @pl.when(jnp.logical_not(is_odd) & (d > 0) & (me >= d))
        def _():
            out_ref[j - 1] = sum_ref[...].astype(BF16)

            @pl.when(gives & hop & (d < span))
            def _():
                give_copy(j - 1).start()

            @pl.when(jnp.logical_not(gives & hop & (d < span)))
            def _():
                total_copy(out_ref, into, t_send, t_recv, j - 1).start()

    def value_hand_out(d):
        hand_out(d, value_parts[rows(d), :], gv_odd, gv_pair, gv_out, dv_buf,
                 gvp_send, gvp_recv, gv_send, gv_in, gv_recv, hops)

    for d in range(span - 1, 0, -2):
        value_hand_out(d)
    for d in range(1, span + 1, 2):
        @pl.when(me >= d)
        def _():
            value_copy(d).wait_recv()

    values_t = values[...].T
    for h in range(heads):
        cols = pl.ds(h * tokens, tokens)
        head = pl.ds(h * width, width)
        attended = (dot_nn(values_t, probs[:, cols]) * row_inv[0:1, cols]).astype(BF16)
        dot = jnp.sum(attended.astype(F32) * gt[:, cols].astype(F32), axis=0, keepdims=True)
        row_dot[:, cols] = jnp.broadcast_to(dot, (8, tokens))
        o_buf[:, head] = attended.T
        if h == heads - 1:
            for d in range(span, -1, -2):
                value_hand_out(d)

    def key_grad_pass(s, carry):
        d = block_at(s)
        if hops:
            @pl.when((s == span) & takes)
            def _():
                give_copy(0).wait_recv()
                take_copy().start()

        value_block = values[rows(d), :]
        for h in range(heads):
            cols = pl.ds(h * tokens, tokens)
            dprob = dot_nn(value_block, gt[:, cols])
            prob = probs[rows(d), cols].astype(F32)
            dscores[rows(d), cols] = (prob * (dprob - row_dot[0:1, cols])).astype(BF16)
        part = dot_nn(dscores[rows(d), :], qs[...]) * scale
        hand_out(d, part, gk_odd, gk_pair, gk_out, dk_buf, gkp_send, gkp_recv, gk_send, gk_in, gk_recv, False)
        return carry

    lax.fori_loop(0, span + 1, key_grad_pass, 0)
    keys_t = keys[...].T
    for h in range(heads):
        cols = pl.ds(h * tokens, tokens)
        grad = (dot_nn(keys_t, dscores[:, cols]) * scale).astype(BF16)
        dq_buf[:, pl.ds(h * width, width)] = grad.T

    for j in range(half - 1, -1, -1):
        @pl.when(me + 2 * (j + 1) < total)
        def _():
            total_copy(gv_out, gv_in, gv_send, gv_recv, j).wait_recv()
            dv_buf[...] += gv_in[j].astype(F32)

    for j in range(half - 1, -1, -1):
        @pl.when(me + 2 * (j + 1) < total)
        def _():
            total_copy(gk_out, gk_in, gk_send, gk_recv, j).wait_recv()
            dk_buf[...] += gk_in[j].astype(F32)


    if hops:
        @pl.when(takes)
        def _():
            take_copy().wait_send()
    for d in range(1, span + 1):
        @pl.when(me + d < total)
        def _():
            seg_copy(d).wait_send()
            if d % 2 == 0:
                key_copy(d).wait_send()
                value_copy(d).wait_send()
    for j in range(half):
        @pl.when(me >= 2 * j + 2 * parity)
        def _():
            key_pass_on(j).wait_send()
            value_pass_on(j).wait_send()

        @pl.when(me >= 2 * j + 1)
        def _():
            pair_copy(gv_odd, gv_pair, gvp_send, gvp_recv, j).wait_send()
            pair_copy(gk_odd, gk_pair, gkp_send, gkp_recv, j).wait_send()

        @pl.when(me >= 2 * j + 2)
        def _():
            total_copy(gv_out, gv_in, gv_send, gv_recv, j).wait_send()
            total_copy(gk_out, gk_in, gk_send, gk_recv, j).wait_send()


def on_device(queries, key_rows, value_rows, out_grad, segment):
    tokens, width = key_rows.shape
    heads = queries.shape[1] // width
    groups = lax.axis_size("grp")
    total = groups * lax.axis_size("seq")
    span = -(-MAXDOC // tokens)
    span += span % 2
    blocks = span + 1
    half = span // 2
    stacked = heads * tokens
    seg_rows = segment.reshape(1, tokens)
    anywhere = pl.BlockSpec(memory_space=pl.ANY)
    sem = pltpu.SemaphoreType.DMA
    block = pltpu.VMEM((half, tokens, width), BF16)
    results = pl.pallas_call(
        functools.partial(kernel, groups, total, span),
        out_shape=(
            pltpu.VMEM(queries.shape, BF16),
            pltpu.VMEM(queries.shape, BF16),
            pltpu.VMEM(key_rows.shape, F32),
            pltpu.VMEM(key_rows.shape, F32),
        ),
        in_specs=[anywhere] * 5,
        out_specs=(pl.BlockSpec(memory_space=pltpu.VMEM),) * 4,
        scratch_shapes=[
            pltpu.VMEM((blocks * tokens, width), BF16),
            pltpu.VMEM((blocks * tokens, width), BF16),
            pltpu.VMEM((blocks, 1, tokens), jnp.int32),
            pltpu.VMEM((stacked, width), BF16),
            pltpu.VMEM((stacked, width), BF16),
            pltpu.VMEM((width, stacked), BF16),
            pltpu.VMEM((width, stacked), BF16),
            pltpu.VMEM((blocks * tokens, width), BF16),
            pltpu.VMEM((width, tokens), BF16),
            pltpu.VMEM((blocks * tokens, stacked), F32),
            pltpu.VMEM((blocks * tokens, stacked), BF16),
            pltpu.VMEM((blocks * tokens, stacked), BF16),
            pltpu.VMEM((blocks * tokens, width), F32),
            pltpu.VMEM((8, stacked), F32),
            pltpu.VMEM((8, stacked), F32),
            pltpu.VMEM((8, stacked), F32),
        ]
        + [block] * 8
        + [pltpu.VMEM((tokens, width), BF16)]
        + [sem((3 + 2 * heads,)), sem, sem]
        + [sem((blocks,))] * 6
        + [sem((half,))] * 10,
        compiler_params=pltpu.CompilerParams(
            collective_id=0, has_side_effects=True, vmem_limit_bytes=48 * 1024 * 1024
        ),
    )(*[
        pltpu.with_memory_space_constraint(a, pltpu.HBM)
        for a in (queries, key_rows, value_rows, out_grad, seg_rows)
    ])
    return write_back(results)


def store(*refs):
    count = (len(refs) - 1) // 2
    copies = [pltpu.make_async_copy(refs[i], refs[count + i], refs[-1].at[i]) for i in range(count)]
    for copy in copies:
        copy.start()
    for copy in copies:
        copy.wait()


def write_back(results):
    anywhere = pl.BlockSpec(memory_space=pl.ANY)
    held = [pltpu.with_memory_space_constraint(r, pltpu.VMEM) for r in results]
    return pl.pallas_call(
        store,
        out_shape=tuple(jax.ShapeDtypeStruct(r.shape, r.dtype) for r in results),
        in_specs=[pl.BlockSpec(memory_space=pltpu.VMEM)] * len(results),
        out_specs=(anywhere,) * len(results),
        scratch_shapes=[pltpu.SemaphoreType.DMA((len(results),))],
        compiler_params=pltpu.CompilerParams(vmem_limit_bytes=4 * 1024 * 1024),
    )(*held)


def solution(mesh):
    in_specs = (P(AXES, None), P(AXES, None), P(AXES, None), P(AXES, None), P(AXES))
    out_specs = (P(AXES, None),) * 4
    return jax.shard_map(
        on_device, mesh=mesh, in_specs=in_specs, out_specs=out_specs, check_vma=False
    )
```
